128 devices in a mesh: segment: 4 (over x_hi, core), strip: 32 (over y, z, x_lo).
Axes of the slice: x: 4 (x_hi: 2, x_lo: 2; x = x_hi * 2 + x_lo), y: 4, z: 4, core: 2. Of those that a mesh axis runs over, the one named last changes fastest.
Arguments:
- features: bfloat16 [2, 256, 512, 256], P(None, 'segment', 'strip'), may hold values from -6 to 6
- weight_first: bfloat16 [3, 3, 256, 256], replicated, may hold values from -0.125 to 0.125
- weight_second: bfloat16 [3, 3, 256, 256], replicated, may hold values from -0.125 to 0.125
- weight_down: bfloat16 [2, 2, 256, 512], replicated, may hold values from -0.1875 to 0.1875
- section_weights: bfloat16 [4, 3, 3, 512, 512], P('segment'), may hold values from -0.09375 to 0.09375
Outputs:
- section_features: bfloat16 [4, 2, 128, 256, 512], P('segment', None, 'strip')
The draws below stay inside these ranges and needn't reach their ends.
All inputs are finite; a program needn't handle non-finite values.
Results may differ from the reference program's by a relative error of at most 0.0095.
Values may be sent and summed in bfloat16 or wider, within the bound.
No kernel may reach another device: no remote copies, remote signals or barrier semaphores. Data moves between devices by JAX's collectives and lax.ppermute only.
A program may use at most 128 MiB of HBM per device.

```python
import jax
import jax.numpy as jnp

C1 = 256
C2 = 512
WINDOWS = 2
SECTIONS = 4
H = 256
W = 512


def level_of(rng, shape, pieces, smallest, high):
    def one(axis_at, shards_of):
        draws = jax.random.uniform(jax.random.fold_in(jax.random.fold_in(rng, 6), axis_at), (shards_of,), jnp.float32, smallest / len(pieces), high / len(pieces))
        return jnp.repeat(jnp.exp(draws), shape[axis_at] // shards_of).reshape((-1,) + (1,) * (len(shape) - axis_at - 1))

    gain = one(*pieces[0])
    for cut in pieces[1:]:
        gain = gain * one(*cut)
    return gain


def bell_draw(rng, extent, scale, bound, shards=(), dtype=jnp.bfloat16):
    entries = scale * jax.random.normal(rng, extent, jnp.float32)
    if shards:
        entries = entries * level_of(rng, extent, shards, -0.22, 0.18)
    return jnp.clip(entries, -bound, bound).astype(dtype)


def setup_inputs(seed: int = 0) -> dict:
    key_list = jax.random.split(jax.random.key(seed), 6)
    features = bell_draw(key_list[0], (WINDOWS, H, W, C1), 1.0, 6.0, ((1, 4), (2, 32)))
    weight_first = bell_draw(key_list[1], (3, 3, C1, C1), (9 * C1) ** -0.5, 0.125)
    weight_second = bell_draw(key_list[2], (3, 3, C1, C1), (9 * C1) ** -0.5, 0.125)
    weight_down = bell_draw(key_list[3], (2, 2, C1, C2), (4 * C1) ** -0.5, 0.1875)
    section_weights = bell_draw(key_list[4], (SECTIONS, 3, 3, C2, C2), (9 * C2) ** -0.5, 0.09375, ((0, 4),))
    return dict(features=features, weight_first=weight_first, weight_second=weight_second, weight_down=weight_down, section_weights=section_weights)


def conv_valid(padded, weight):
    batches, rows_pad, columns_pad, channels = padded.shape
    rows = rows_pad - 2
    columns = columns_pad - 2
    total = None
    for row_off in range(3):
        for col_off in range(3):
            window = padded[:, row_off:row_off + rows, col_off:col_off + columns, :].reshape(-1, channels)
            partial_sum = jnp.dot(window, weight[row_off, col_off], preferred_element_type=jnp.float32)
            total = partial_sum if total is None else total + partial_sum
    return total.reshape(batches, rows, columns, weight.shape[3])


def residual_layer(inputs, weight):
    padded = jnp.pad(inputs, ((0, 0), (1, 1), (1, 1), (0, 0)))
    return jax.nn.relu(inputs.astype(jnp.float32) + conv_valid(padded, weight)).astype(jnp.bfloat16)


def reference(features, weight_first, weight_second, weight_down, section_weights):
    first = residual_layer(features, weight_first)
    second = residual_layer(first, weight_second)
    batches, rows, columns, channels = second.shape
    blocks = second.reshape(batches, rows // 2, 2, columns // 2, 2, channels)
    total = None
    for row_off in range(2):
        for col_off in range(2):
            piece = blocks[:, :, row_off, :, col_off, :].reshape(-1, channels)
            partial_sum = jnp.dot(piece, weight_down[row_off, col_off], preferred_element_type=jnp.float32)
            total = partial_sum if total is None else total + partial_sum
    current = jax.nn.relu(total).reshape(batches, rows // 2, columns // 2, weight_down.shape[3]).astype(jnp.bfloat16)
    stacked = []
    for section in range(SECTIONS):
        current = residual_layer(current, section_weights[section])
        stacked.append(current)
    return jnp.stack(stacked)
```

```python
import functools

import jax
import jax.numpy as jnp
from jax import lax
from jax.experimental import pallas as pl
from jax.experimental.pallas import tpu as pltpu
from jax.sharding import PartitionSpec as P

AXES = ("segment", "strip")
F32 = jnp.float32
BF16 = jnp.bfloat16
VMEM = pltpu.VMEM


def vmem_spec():
    return pl.BlockSpec(memory_space=pltpu.VMEM)


def smem_spec():
    return pl.BlockSpec(memory_space=pltpu.SMEM)


def any_spec():
    return pl.BlockSpec(memory_space=pl.ANY)


def stem_kernel(place, feat, up, down, left, right, w1, w2, wd, out, s1, x1, s2, x2, s3, dbuf):
    halo = 6
    rows = feat.shape[0]
    cols = feat.shape[1]
    ch = feat.shape[2]
    full = rows + 2 * halo
    row_base = place[0]
    total_rows = place[1]
    left_edge = place[2]
    right_edge = place[3]
    pitch = s1.shape[1] // full
    width = cols + 8
    lanes = s1.shape[2]

    s1d = s1.reshape(ch // lanes, full, pitch, lanes)
    for k in range(ch // lanes):
        at = slice(k * lanes, (k + 1) * lanes)
        s1d[k, 0:halo, 8 : 8 + cols, :] = up[:, :, at].astype(F32)
        s1d[k, halo : halo + rows, 8 : 8 + cols, :] = feat[:, :, at].astype(F32)
        s1d[k, halo + rows : full, 8 : 8 + cols, :] = down[:, :, at].astype(F32)
        for j in range(2):
            s1[k, pl.ds(6 + j, full, stride=pitch), :] = left[j, :, at].astype(F32)
            s1[k, pl.ds(8 + cols + j, full, stride=pitch), :] = right[j, :, at].astype(F32)

    step = 19

    def shift1(i, carry):
        r = i * step
        for c in range(3):
            for k in range(ch // lanes):
                x1[pl.ds(r, step), :, c * ch + k * lanes : c * ch + (k + 1) * lanes] = s1d[
                    k, pl.ds(r, step), 6 + c : 6 + c + width, :
                ].astype(BF16)
        return carry

    lax.fori_loop(0, full // step, shift1, 0)

    out1 = full - 2
    block1 = 37
    s2d = s2.reshape(out1, pitch, ch)

    def layer1(i, carry):
        r = i * block1
        acc = None
        for a in range(3):
            part = jnp.dot(
                x1[pl.ds(r + a, block1)].reshape(block1 * width, 3 * ch),
                w1[a],
                preferred_element_type=F32,
            )
            acc = part if acc is None else acc + part
        acc = acc.reshape(block1, width, ch)
        y = jnp.maximum(acc + x1[pl.ds(r + 1, block1), :, ch : 2 * ch].astype(F32), 0.0)
        row = row_base + 1 + r + lax.broadcasted_iota(jnp.int32, (block1, width, 1), 0)
        col = lax.broadcasted_iota(jnp.int32, (block1, width, 1), 1) - 1
        ok = (row >= 0) & (row < total_rows)
        ok = ok & ((col >= 0) | (left_edge == 0)) & ((col < cols) | (right_edge == 0))
        y = jnp.where(ok, y, 0.0)
        s2d[pl.ds(r, block1), 8 : 8 + width, :] = y.astype(BF16).astype(F32)
        return carry

    lax.fori_loop(0, out1 // block1, layer1, 0)

    def shift2(i, carry):
        r = i * block1
        for c in range(3):
            x2[pl.ds(r, block1), :, c * ch : (c + 1) * ch] = s2d[
                pl.ds(r, block1), 8 + c : 8 + c + cols, :
            ].astype(BF16)
        return carry

    lax.fori_loop(0, out1 // block1, shift2, 0)

    out2 = out1 - 2
    block2 = 36

    def layer2(i, carry):
        r = i * block2
        acc = None
        for a in range(3):
            part = jnp.dot(
                x2[pl.ds(r + a, block2)].reshape(block2 * cols, 3 * ch),
                w2[a],
                preferred_element_type=F32,
            )
            acc = part if acc is None else acc + part
        res = x2[pl.ds(r + 1, block2), :, ch : 2 * ch].reshape(block2 * cols, ch).astype(F32)
        y = jnp.maximum(acc + res, 0.0)
        y = y.astype(BF16).astype(F32)
        for k in range(ch // lanes):
            s3[k, pl.ds(i * (block2 * cols), block2 * cols), :] = y[:, k * lanes : (k + 1) * lanes]
        return carry

    lax.fori_loop(0, out2 // block2, layer2, 0)

    zrows = out2 // 2
    zcols = cols // 2

    for a in range(2):
        for c in range(2):
            for k in range(ch // lanes):
                at = (a * 2 + c) * ch + k * lanes
                for i in range(zrows):
                    dbuf[i * zcols : (i + 1) * zcols, at : at + lanes] = s3[
                        k, pl.ds((2 * i + a) * cols + c, zcols, stride=2), :
                    ].astype(BF16)
    z = jnp.maximum(jnp.dot(dbuf[...], wd[...], preferred_element_type=F32), 0.0)
    z = z.reshape(zrows, zcols, z.shape[-1])
    zrow = row_base // 2 + 1 + lax.broadcasted_iota(jnp.int32, (zrows, zcols, 1), 0)
    z = jnp.where((zrow >= 0) & (zrow < total_rows // 2), z, 0.0).astype(BF16)
    slots = out.shape[0]
    depth = out.shape[1]
    own = (zrows - 4) // slots
    for b in range(slots):
        out[b] = z[own * b : own * b + depth]


def stem(place, feat, up, down, left, right, w1, w2, wd, slots):
    rows, cols, ch = feat.shape
    full = rows + 12
    out_ch = wd.shape[1]
    own = rows // 2 // slots
    flops = 2 * (74 * 24 + 72 * 16) * 9 * ch * ch
    return pl.pallas_call(
        stem_kernel,
        out_shape=jax.ShapeDtypeStruct((slots, own + 4, cols // 2, out_ch), BF16),
        in_specs=[smem_spec()] + [vmem_spec()] * 8,
        out_specs=vmem_spec(),
        scratch_shapes=[
            VMEM((ch // 128, full * 32, 128), F32),
            VMEM((full, 24, 3 * ch), BF16),
            VMEM(((full - 2) * 32, ch), F32),
            VMEM((full - 2, 16, 3 * ch), BF16),
            VMEM((ch // 128, (full - 4) * 16, 128), F32),
            VMEM(((full - 4) // 2 * 8, 4 * ch), BF16),
        ],
        compiler_params=pltpu.CompilerParams(vmem_limit_bytes=48 * 2**20),
        cost_estimate=pl.CostEstimate(flops=flops, bytes_accessed=4 * 2**20, transcendentals=0),
        name="stem",
    )(place, feat, up, down, left, right, w1, w2, wd)


EDGE = 8


def duo_body(place, fill, own_w, peer_w, keep, send, full, scratch, window):
    s1, x1, s2, x2, wa, wb, za, zb, zf, sems = scratch
    core = place[1]
    row0, row_total, col0, col_total = place[2], place[3], place[4], place[5]
    rows_in, width, wide = x1.shape
    ch = wide // 3

    @pl.when(core == 0)
    def _():
        pltpu.make_async_copy(own_w, wa, sems.at[0]).start()
        pltpu.make_async_copy(peer_w, wb, sems.at[1]).start()

    @pl.when(core == 1)
    def _():
        pltpu.make_async_copy(peer_w, wa, sems.at[0]).start()
        pltpu.make_async_copy(own_w, wb, sems.at[1]).start()

    fill(s1)

    def shift(src, dst):
        def go(r, carry):
            for c in range(3):
                dst[r, :, c * ch : (c + 1) * ch] = src[
                    r, EDGE - 1 + c : EDGE - 1 + c + width, :
                ].astype(BF16)
            return carry

        lax.fori_loop(0, dst.shape[0], go, 0)

    def layer(x, w, r, first_row):
        acc = None
        for a in range(3):
            part = jnp.dot(
                x[pl.ds(r + a, 2)].reshape(2 * width, 3 * ch), w[a], preferred_element_type=F32
            )
            acc = part if acc is None else acc + part
        acc = acc.reshape(2, width, ch)
        y = jnp.maximum(acc + x[pl.ds(r + 1, 2), :, ch : 2 * ch].astype(F32), 0.0)
        row = first_row + r + lax.broadcasted_iota(jnp.int32, (2, width, 1), 0)
        col = col0 + lax.broadcasted_iota(jnp.int32, (2, width, 1), 1)
        ok = (row >= 0) & (row < row_total) & (col >= 0) & (col < col_total)
        return jnp.where(ok, y, 0.0).astype(BF16)

    shift(s1, x1)
    pltpu.make_async_copy(own_w, wa, sems.at[0]).wait()
    rows_mid = rows_in - 2

    def first(i, carry):
        r = 2 * i
        y = layer(x1, wa, r, row0 + 1)
        s2[pl.ds(r, 2), EDGE : EDGE + width, :] = y.astype(F32)
        return carry

    lax.fori_loop(0, rows_mid // 2, first, 0)
    shift(s2, x2)
    rows_out = rows_mid - 2
    za[...] = x2[1 : 1 + rows_out, EDGE : width - EDGE, ch : 2 * ch]
    pltpu.make_async_copy(own_w, wb, sems.at[1]).wait()

    def second(i, carry):
        r = 2 * i
        y = layer(x2, wb, r, row0 + 2)
        zf[pl.ds(r, 2)] = y
        return carry

    lax.fori_loop(0, rows_out // 2, second, 0)
    zb[...] = zf[:, EDGE : width - EDGE, :]

    half = width - 2 * EDGE

    @pl.when(core == 0)
    def _():
        pltpu.make_async_copy(za, keep.at[window, :, pl.ds(0, half), :], sems.at[2]).start()
        pltpu.make_async_copy(zb, send.at[window], sems.at[3]).start()

    @pl.when(core == 1)
    def _():
        pltpu.make_async_copy(zb, keep.at[window, :, pl.ds(half, half), :], sems.at[2]).start()
        pltpu.make_async_copy(za, send.at[window], sems.at[3]).start()

    if full is not None:
        copy = pltpu.make_async_copy(zf, full, sems.at[4])
        copy.start()
        copy.wait()
    pltpu.make_async_copy(za, keep.at[window, :, pl.ds(0, half), :], sems.at[2]).wait()
    pltpu.make_async_copy(zb, send.at[window], sems.at[3]).wait()


def clear_edges(s, width):
    rows = s.shape[0]
    s[:, 0:EDGE, :] = jnp.zeros((rows, EDGE, s.shape[2]), F32)
    s[:, EDGE + width :, :] = jnp.zeros((rows, EDGE, s.shape[2]), F32)


def early_kernel(window, chained, *refs):
    place, lo, hi, side, own_w, peer_w = refs[:6]
    refs = refs[6 + (2 if chained else 0) :]
    keep, send, full = refs[:3]
    scratch = refs[3:]
    s1, x1, s2 = scratch[0], scratch[1], scratch[2]
    width = x1.shape[1]
    block = lo.shape[2]

    def fill(s):
        clear_edges(s, width)
        clear_edges(s2, width)
        parts = lo.shape[0]

        def row(r, carry):
            for e in range(parts):
                at = 2 * EDGE + block * e
                s[r, at : at + block, :] = lo[e, r].astype(F32)
                at = at + block * parts
                s[r, at : at + block, :] = hi[e, r].astype(F32)
            on_left = place[1] == 1
            edge = side[r].astype(F32)
            s[r, EDGE : 2 * EDGE, :] = jnp.where(on_left, edge, 0.0)
            s[r, width : width + EDGE, :] = jnp.where(on_left, 0.0, edge)
            return carry

        lax.fori_loop(0, s.shape[0], row, 0)

    @pl.when(place[0] == 1)
    def _():
        duo_body(place, fill, own_w, peer_w, keep, send, full, scratch, window)


def late_kernel(window, *refs):
    place, above, main, below, own_w, peer_w, _, _ = refs[:8]
    keep, send = refs[8:10]
    scratch = refs[10:]
    x1, s2 = scratch[1], scratch[2]
    width = x1.shape[1]

    def fill(s):
        clear_edges(s, width)
        clear_edges(s2, width)
        rim = above.shape[0]
        mid = main.shape[0]
        s[0:rim, EDGE : EDGE + width, :] = above[...].astype(F32)
        s[rim : rim + mid, EDGE : EDGE + width, :] = main[...].astype(F32)
        s[rim + mid :, EDGE : EDGE + width, :] = below[...].astype(F32)

    @pl.when(place[0] == 1)
    def _():
        duo_body(place, fill, own_w, peer_w, keep, send, None, scratch, window)


def duo_scratch(rows, width, ch):
    return [
        VMEM((rows + 4, width + 2 * EDGE, ch), F32),
        VMEM((rows + 4, width, 3 * ch), BF16),
        VMEM((rows + 2, width + 2 * EDGE, ch), F32),
        VMEM((rows + 2, width, 3 * ch), BF16),
        VMEM((3, 3 * ch, ch), BF16),
        VMEM((3, 3 * ch, ch), BF16),
        VMEM((rows, width - 2 * EDGE, ch), BF16),
        VMEM((rows, width - 2 * EDGE, ch), BF16),
        VMEM((rows, width, ch), BF16),
        pltpu.SemaphoreType.DMA((5,)),
    ]


def duo_params(rows, width, ch):
    flops = 2 * (2 * rows + 2) * width * 9 * ch * ch
    return dict(
        compiler_params=pltpu.CompilerParams(vmem_limit_bytes=48 * 2**20),
        cost_estimate=pl.CostEstimate(flops=flops, bytes_accessed=12 * 2**20, transcendentals=0),
    )


def early(window, place, lo, hi, side, own_w, peer_w, buffers, windows, rows, half):
    ch = lo.shape[-1]
    width = half + 2 * EDGE
    chained = buffers is not None
    return pl.pallas_call(
        functools.partial(early_kernel, window, chained),
        out_shape=(
            jax.ShapeDtypeStruct((windows, rows, 2 * half, ch), BF16),
            jax.ShapeDtypeStruct((windows, rows, half, ch), BF16),
            jax.ShapeDtypeStruct((rows, width, ch), BF16),
        ),
        in_specs=[smem_spec()] + [vmem_spec()] * 3 + [any_spec()] * (4 if chained else 2),
        out_specs=(any_spec(), any_spec(), any_spec()),
        scratch_shapes=duo_scratch(rows, width, ch),
        input_output_aliases={6: 0, 7: 1} if chained else {},
        name=f"early{window}",
        **duo_params(rows, width, ch),
    )(place, lo, hi, side, own_w, peer_w, *(buffers or ()))


def late(window, place, above, main, below, own_w, peer_w, buffers):
    rows, width, ch = main.shape
    return pl.pallas_call(
        functools.partial(late_kernel, window),
        out_shape=tuple(jax.ShapeDtypeStruct(b.shape, b.dtype) for b in buffers),
        in_specs=[smem_spec()] + [vmem_spec()] * 3 + [any_spec()] * 4,
        out_specs=(any_spec(), any_spec()),
        scratch_shapes=duo_scratch(rows, width, ch),
        input_output_aliases={6: 0, 7: 1},
        name=f"late{window}",
        **duo_params(rows, width, ch),
    )(place, above, main, below, own_w, peer_w, *buffers)


def shards(features, weight_first, weight_second, weight_down, section_weights):
    segments = lax.axis_size("segment")
    strips = lax.axis_size("strip")
    seg = lax.axis_index("segment")
    strip = lax.axis_index("strip")
    windows, tile_rows, tile_cols, c1 = features.shape
    c2 = weight_down.shape[3]
    group = strips // segments
    strip_rows = segments * tile_rows // 2 // strips
    total_cols = strips * tile_cols // 2
    half = total_cols // 2
    core = lax.rem(seg, 2)
    far = seg // 2
    i32 = jnp.int32

    def device(s, c):
        return s * strips + c

    own_w = section_weights.reshape(3, 3 * c2, c2)
    peer_w = lax.ppermute(own_w, "segment", [(s, s ^ 1) for s in range(segments)])

    rim_r, rim_c = 6, 2
    ahead = [(s, s + 1) for s in range(segments - 1)]
    back = [(b, a) for a, b in ahead]
    up = lax.ppermute(features[:, tile_rows - rim_r :], "segment", ahead)
    down = lax.ppermute(features[:, :rim_r], "segment", back)

    def side(sl):
        piece = jnp.concatenate([up[:, :, sl], features[:, :, sl], down[:, :, sl]], axis=1)
        return jnp.swapaxes(piece, 1, 2)

    along = [(c, c + 1) for c in range(strips - 1)]
    against = [(b, a) for a, b in along]
    left = lax.ppermute(side(slice(tile_cols - rim_c, tile_cols)), "strip", along)
    right = lax.ppermute(side(slice(0, rim_c)), "strip", against)

    stem_place = jnp.stack(
        [
            seg * tile_rows - rim_r,
            i32(segments * tile_rows),
            (strip == 0).astype(i32),
            (strip == strips - 1).astype(i32),
        ]
    ).astype(i32)
    w1 = weight_first.reshape(3, 3 * c1, c1)
    w2 = weight_second.reshape(3, 3 * c1, c1)
    wd = weight_down.reshape(4 * c1, c2)

    groups = [[g * group + i for i in range(group)] for g in range(segments)]
    low, high, edge = [], [], []
    for s in range(segments):
        for d in range(segments):
            for b in range(group):
                src, dst = device(s, d * group + b), device(d // 2, s * group + b)
                (low if d % 2 == 0 else high).append((src, dst))
                if d == 2:
                    edge.append((src, device(0, s * group + b)))
                if d == 1:
                    edge.append((src, device(1, s * group + b)))
    quarter = strip // group

    tiles = []
    for w in range(windows):
        z = stem(stem_place, features[w], up[w], down[w], left[w], right[w], w1, w2, wd, group)
        shape = z.shape
        got = lax.all_to_all(
            z.reshape(-1, *shape[2:]), "strip", 0, 0, axis_index_groups=groups, tiled=True
        ).reshape(shape)
        lo = lax.ppermute(got, AXES, low)
        hi = lax.ppermute(got, AXES, high)
        pick = jnp.where(quarter == 2, got[0], got[group - 1])
        tiles.append((lo, hi, lax.ppermute(pick, AXES, edge)))

    common = [
        core,
        strip * strip_rows - 2,
        i32(segments * tile_rows // 2),
        core * half - EDGE,
        i32(total_cols),
    ]
    early_place = jnp.stack([(far == 0).astype(i32), *common]).astype(i32)
    late_place = jnp.stack([(far == 1).astype(i32), *common]).astype(i32)

    buffers = None
    passed = []
    across = [
        (device(h, t), device(h + 2, t)) for h in range(2) for t in range(strips)
    ]
    for w in range(windows):
        keep, send, full = early(
            w, early_place, *tiles[w], own_w, peer_w, buffers, windows, strip_rows, half
        )
        buffers = (keep, send)
        passed.append(lax.ppermute(full, AXES, across))
    later = [(device(s, a), device(s, b)) for s in (2, 3) for a, b in along]
    sooner = [(b, a) for a, b in later]
    for w in range(windows):
        main = passed[w]
        above = lax.ppermute(main[strip_rows - 2 :], AXES, later)
        below = lax.ppermute(main[:2], AXES, sooner)
        buffers = late(w, late_place, above, main, below, own_w, peer_w, buffers)
    keep, send = buffers
    other = lax.ppermute(send, "segment", [(s, s ^ 1) for s in range(segments)])
    zero = i32(0)
    result = lax.dynamic_update_slice(keep, other, (zero, zero, (1 - core) * half, zero))
    return result[None]


def solution(mesh):
    return jax.shard_map(
        shards,
        mesh=mesh,
        in_specs=(
            P(None, "segment", "strip", None),
            P(),
            P(),
            P(),
            P("segment", None, None, None, None),
        ),
        out_specs=P("segment", None, "strip", None, None),
        check_vma=False,
    )
```

```python
import functools

import jax
import jax.numpy as jnp
from jax import lax
from jax.experimental import pallas as pl
from jax.experimental.pallas import tpu as pltpu
from jax.sharding import PartitionSpec as P

AXES = ("segment", "strip")
F32 = jnp.float32
BF16 = jnp.bfloat16
VMEM = pltpu.VMEM


def vmem_spec():
    return pl.BlockSpec(memory_space=pltpu.VMEM)


def smem_spec():
    return pl.BlockSpec(memory_space=pltpu.SMEM)


def hbm_spec():
    return pl.BlockSpec(memory_space=pltpu.HBM)


def any_spec():
    return pl.BlockSpec(memory_space=pl.ANY)


def pack_kernel(feat, top, bottom, first_cols, last_cols, wide):
    windows, rows, cols, ch = feat.shape
    rim_r, rim_c = top.shape[1], first_cols.shape[1]
    lanes = wide.shape[2]
    top[...] = feat[:, :rim_r]
    bottom[...] = feat[:, rows - rim_r :]
    for k in range(ch // lanes):
        at = slice(k * lanes, (k + 1) * lanes)
        wide[k] = feat[:, :, :, at].astype(F32).reshape(windows * rows * cols, lanes)
        for w in range(windows):
            for j in range(rim_c):
                base = w * rows * cols
                first_cols[w, j, :, at] = wide[k, pl.ds(base + j, rows, stride=cols), :].astype(BF16)
                last_cols[w, j, :, at] = wide[
                    k, pl.ds(base + cols - rim_c + j, rows, stride=cols), :
                ].astype(BF16)


def pack(features, rim_r, rim_c):
    windows, rows, cols, ch = features.shape
    row_shape = jax.ShapeDtypeStruct((windows, rim_r, cols, ch), BF16)
    col_shape = jax.ShapeDtypeStruct((windows, rim_c, rows, ch), BF16)
    return pl.pallas_call(
        pack_kernel,
        out_shape=(row_shape, row_shape, col_shape, col_shape),
        in_specs=[vmem_spec()],
        out_specs=(vmem_spec(),) * 4,
        scratch_shapes=[VMEM((ch // 128, windows * rows * cols, 128), F32)],
        compiler_params=pltpu.CompilerParams(vmem_limit_bytes=24 * 2**20),
        name="pack",
    )(features)


def stem_kernel(window, place, feat, up, down, left, right, w1_in, w2_in, wd_in, out, *scratch):
    s1, x1, s2, x2, s3, dbuf, w1, w2, wd, sems = scratch
    pairs = ((w1_in, w1), (w2_in, w2), (wd_in, wd))
    copies = [pltpu.make_async_copy(*pair, sems.at[i]) for i, pair in enumerate(pairs)]
    for copy in copies:
        copy.start()
    halo = 6
    _, rows, cols, ch = feat.shape
    full = rows + 2 * halo
    row_base = place[0]
    total_rows = place[1]
    left_edge = place[2]
    right_edge = place[3]
    pitch = s1.shape[1] // full
    width = cols + 8
    lanes = s1.shape[2]

    s1d = s1.reshape(ch // lanes, full, pitch, lanes)
    for k in range(ch // lanes):
        at = slice(k * lanes, (k + 1) * lanes)
        s1d[k, 0:halo, 8 : 8 + cols, :] = up[window, :, :, at].astype(F32)
        s1d[k, halo : halo + rows, 8 : 8 + cols, :] = feat[window, :, :, at].astype(F32)
        s1d[k, halo + rows : full, 8 : 8 + cols, :] = down[window, :, :, at].astype(F32)
        for src, to in ((left, 6), (right, 8 + cols)):
            for j in range(2):
                for take, put, count in (
                    (0, halo, rows),
                    (rows, 0, halo),
                    (rows + halo, halo + rows, halo),
                ):
                    s1[k, pl.ds(put * pitch + to + j, count, stride=pitch), :] = src[
                        window, j, take : take + count, at
                    ].astype(F32)

    step = 19

    def shift1(i, carry):
        r = i * step
        for c in range(3):
            for k in range(ch // lanes):
                x1[pl.ds(r, step), :, c * ch + k * lanes : c * ch + (k + 1) * lanes] = s1d[
                    k, pl.ds(r, step), 6 + c : 6 + c + width, :
                ].astype(BF16)
        return carry

    lax.fori_loop(0, full // step, shift1, 0)
    copies[0].wait()

    out1 = full - 2
    block1 = 37
    s2d = s2.reshape(out1, pitch, ch)

    def layer1(i, carry):
        r = i * block1
        acc = None
        for a in range(3):
            part = jnp.dot(
                x1[pl.ds(r + a, block1)].reshape(block1 * width, 3 * ch),
                w1[a],
                preferred_element_type=F32,
            )
            acc = part if acc is None else acc + part
        acc = acc.reshape(block1, width, ch)
        y = jnp.maximum(acc + x1[pl.ds(r + 1, block1), :, ch : 2 * ch].astype(F32), 0.0)
        row = row_base + 1 + r + lax.broadcasted_iota(jnp.int32, (block1, width, 1), 0)
        col = lax.broadcasted_iota(jnp.int32, (block1, width, 1), 1) - 1
        ok = (row >= 0) & (row < total_rows)
        ok = ok & ((col >= 0) | (left_edge == 0)) & ((col < cols) | (right_edge == 0))
        y = jnp.where(ok, y, 0.0)
        s2d[pl.ds(r, block1), 8 : 8 + width, :] = y.astype(BF16).astype(F32)
        return carry

    lax.fori_loop(0, out1 // block1, layer1, 0)

    def shift2(i, carry):
        r = i * block1
        for c in range(3):
            x2[pl.ds(r, block1), :, c * ch : (c + 1) * ch] = s2d[
                pl.ds(r, block1), 8 + c : 8 + c + cols, :
            ].astype(BF16)
        return carry

    lax.fori_loop(0, out1 // block1, shift2, 0)
    copies[1].wait()

    out2 = out1 - 2
    block2 = 36

    def layer2(i, carry):
        r = i * block2
        acc = None
        for a in range(3):
            part = jnp.dot(
                x2[pl.ds(r + a, block2)].reshape(block2 * cols, 3 * ch),
                w2[a],
                preferred_element_type=F32,
            )
            acc = part if acc is None else acc + part
        res = x2[pl.ds(r + 1, block2), :, ch : 2 * ch].reshape(block2 * cols, ch).astype(F32)
        y = jnp.maximum(acc + res, 0.0)
        y = y.astype(BF16).astype(F32)
        for k in range(ch // lanes):
            s3[k, pl.ds(i * (block2 * cols), block2 * cols), :] = y[:, k * lanes : (k + 1) * lanes]
        return carry

    lax.fori_loop(0, out2 // block2, layer2, 0)

    zrows = out2 // 2
    zcols = cols // 2

    for a in range(2):
        for c in range(2):
            for k in range(ch // lanes):
                at = (a * 2 + c) * ch + k * lanes
                for i in range(zrows):
                    dbuf[i * zcols : (i + 1) * zcols, at : at + lanes] = s3[
                        k, pl.ds((2 * i + a) * cols + c, zcols, stride=2), :
                    ].astype(BF16)
    copies[2].wait()
    z = jnp.maximum(jnp.dot(dbuf[...], wd[...], preferred_element_type=F32), 0.0)
    z = z.reshape(zrows, zcols, z.shape[-1])
    zrow = row_base // 2 + 1 + lax.broadcasted_iota(jnp.int32, (zrows, zcols, 1), 0)
    z = jnp.where((zrow >= 0) & (zrow < total_rows // 2), z, 0.0).astype(BF16)
    slots = out.shape[0]
    depth = out.shape[1]
    own = (zrows - 4) // slots
    for b in range(slots):
        out[b] = z[own * b : own * b + depth]


def stem(window, place, feat, up, down, left, right, w1, w2, wd, slots):
    _, rows, cols, ch = feat.shape
    full = rows + 12
    out_ch = wd.shape[1]
    own = rows // 2 // slots
    flops = 2 * (74 * 24 + 72 * 16) * 9 * ch * ch
    return pl.pallas_call(
        functools.partial(stem_kernel, window),
        out_shape=jax.ShapeDtypeStruct((slots, own + 4, cols // 2, out_ch), BF16),
        in_specs=[smem_spec()] + [vmem_spec()] * 5 + [hbm_spec()] * 3,
        out_specs=vmem_spec(),
        scratch_shapes=[
            VMEM((ch // 128, full * 32, 128), F32),
            VMEM((full, 24, 3 * ch), BF16),
            VMEM(((full - 2) * 32, ch), F32),
            VMEM((full - 2, 16, 3 * ch), BF16),
            VMEM((ch // 128, (full - 4) * 16, 128), F32),
            VMEM(((full - 4) // 2 * 8, 4 * ch), BF16),
            VMEM(w1.shape, BF16),
            VMEM(w2.shape, BF16),
            VMEM(wd.shape, BF16),
            pltpu.SemaphoreType.DMA((3,)),
        ],
        compiler_params=pltpu.CompilerParams(vmem_limit_bytes=48 * 2**20),
        cost_estimate=pl.CostEstimate(flops=flops, bytes_accessed=4 * 2**20, transcendentals=0),
    )(place, feat, up, down, left, right, w1, w2, wd)


EDGE = 8


def duo_body(place, fill, own_w, peer_w, keep, send, full, scratch, window):
    s1, x1, s2, x2, wa, wb, za, zb, zf, sems = scratch
    core = place[1]

    def load(mine, dst, sem):
        @pl.when(core == mine)
        def _():
            pltpu.make_async_copy(own_w, dst, sem).start()

        @pl.when(core != mine)
        def _():
            pltpu.make_async_copy(peer_w, dst, sem).start()

    load(0, wa, sems.at[3])
    row0, row_total, col0, col_total = place[2], place[3], place[4], place[5]
    rows_in, width, wide = x1.shape
    ch = wide // 3

    fill(s1)

    def shift(src, dst):
        def go(r, carry):
            for c in range(3):
                dst[r, :, c * ch : (c + 1) * ch] = src[
                    r, EDGE - 1 + c : EDGE - 1 + c + width, :
                ].astype(BF16)
            return carry

        lax.fori_loop(0, dst.shape[0], go, 0)

    def layer(x, w, r, first_row):
        acc = None
        for a in range(3):
            part = jnp.dot(
                x[pl.ds(r + a, 2)].reshape(2 * width, 3 * ch), w[a], preferred_element_type=F32
            )
            acc = part if acc is None else acc + part
        acc = acc.reshape(2, width, ch)
        y = jnp.maximum(acc + x[pl.ds(r + 1, 2), :, ch : 2 * ch].astype(F32), 0.0)
        row = first_row + r + lax.broadcasted_iota(jnp.int32, (2, width, 1), 0)
        col = col0 + lax.broadcasted_iota(jnp.int32, (2, width, 1), 1)
        ok = (row >= 0) & (row < row_total) & (col >= 0) & (col < col_total)
        return jnp.where(ok, y, 0.0).astype(BF16)

    shift(s1, x1)
    pltpu.make_async_copy(own_w, wa, sems.at[3]).wait()
    load(1, wb, sems.at[4])
    rows_mid = rows_in - 2

    def first(i, carry):
        r = 2 * i
        y = layer(x1, wa, r, row0 + 1)
        s2[pl.ds(r, 2), EDGE : EDGE + width, :] = y.astype(F32)
        return carry

    lax.fori_loop(0, rows_mid // 2, first, 0)
    shift(s2, x2)
    rows_out = rows_mid - 2
    za[...] = x2[1 : 1 + rows_out, EDGE : width - EDGE, ch : 2 * ch]
    half = width - 2 * EDGE

    @pl.when(core == 0)
    def _():
        pltpu.make_async_copy(za, keep.at[window, :, pl.ds(0, half), :], sems.at[0]).start()

    @pl.when(core == 1)
    def _():
        pltpu.make_async_copy(za, send, sems.at[0]).start()

    pltpu.make_async_copy(own_w, wb, sems.at[4]).wait()

    def second(i, carry):
        r = 2 * i
        zf[pl.ds(r, 2)] = layer(x2, wb, r, row0 + 2)
        return carry

    lax.fori_loop(0, rows_out // 2, second, 0)

    if full is not None:
        pltpu.make_async_copy(zf, full, sems.at[2]).start()
    zb[...] = zf[:, EDGE : width - EDGE, :]

    @pl.when(core == 0)
    def _():
        pltpu.make_async_copy(zb, send, sems.at[1]).start()
        pltpu.make_async_copy(za, keep.at[window, :, pl.ds(0, half), :], sems.at[0]).wait()
        pltpu.make_async_copy(zb, send, sems.at[1]).wait()

    @pl.when(core == 1)
    def _():
        pltpu.make_async_copy(zb, keep.at[window, :, pl.ds(half, half), :], sems.at[1]).start()
        pltpu.make_async_copy(za, send, sems.at[0]).wait()
        pltpu.make_async_copy(zb, keep.at[window, :, pl.ds(half, half), :], sems.at[1]).wait()

    if full is not None:
        pltpu.make_async_copy(zf, full, sems.at[2]).wait()


def clear_edges(s, width):
    rows = s.shape[0]
    s[:, 0:EDGE, :] = jnp.zeros((rows, EDGE, s.shape[2]), F32)
    s[:, EDGE + width :, :] = jnp.zeros((rows, EDGE, s.shape[2]), F32)


def early_kernel(window, chained, *refs):
    place, lo, hi, side, own_w, peer_w = refs[:6]
    refs = refs[6 + (1 if chained else 0) :]
    keep, send, full = refs[:3]
    scratch = refs[3:]
    x1, s2 = scratch[1], scratch[2]
    width = x1.shape[1]
    block = lo.shape[2]

    def fill(s):
        clear_edges(s, width)
        clear_edges(s2, width)
        parts = lo.shape[0]

        def row(r, carry):
            for e in range(parts):
                at = 2 * EDGE + block * e
                s[r, at : at + block, :] = lo[e, r].astype(F32)
                at = at + block * parts
                s[r, at : at + block, :] = hi[e, r].astype(F32)
            on_left = place[1] == 1
            edge = side[r].astype(F32)
            s[r, EDGE : 2 * EDGE, :] = jnp.where(on_left, edge, 0.0)
            s[r, width : width + EDGE, :] = jnp.where(on_left, 0.0, edge)
            return carry

        lax.fori_loop(0, s.shape[0], row, 0)

    @pl.when(place[0] == 1)
    def _():
        duo_body(place, fill, own_w, peer_w, keep, send, full, scratch, window)


def late_kernel(window, *refs):
    place, above, main, below, own_w, peer_w, _, _ = refs[:8]
    keep, send = refs[8:10]
    scratch = refs[10:]
    x1, s2 = scratch[1], scratch[2]
    width = x1.shape[1]

    def fill(s):
        clear_edges(s, width)
        clear_edges(s2, width)
        rim = above.shape[0]
        mid = main.shape[0]
        s[0:rim, EDGE : EDGE + width, :] = above[...].astype(F32)
        s[rim : rim + mid, EDGE : EDGE + width, :] = main[...].astype(F32)
        s[rim + mid :, EDGE : EDGE + width, :] = below[...].astype(F32)

    @pl.when(place[0] == 1)
    def _():
        duo_body(place, fill, own_w, peer_w, keep, send, None, scratch, window)


def duo_scratch(rows, width, ch):
    return [
        VMEM((rows + 4, width + 2 * EDGE, ch), F32),
        VMEM((rows + 4, width, 3 * ch), BF16),
        VMEM((rows + 2, width + 2 * EDGE, ch), F32),
        VMEM((rows + 2, width, 3 * ch), BF16),
        VMEM((3, 3 * ch, ch), BF16),
        VMEM((3, 3 * ch, ch), BF16),
        VMEM((rows, width - 2 * EDGE, ch), BF16),
        VMEM((rows, width - 2 * EDGE, ch), BF16),
        VMEM((rows, width, ch), BF16),
        pltpu.SemaphoreType.DMA((5,)),
    ]


def duo_params(rows, width, ch):
    flops = 2 * (2 * rows + 2) * width * 9 * ch * ch
    return dict(
        compiler_params=pltpu.CompilerParams(vmem_limit_bytes=48 * 2**20),
        cost_estimate=pl.CostEstimate(flops=flops, bytes_accessed=12 * 2**20, transcendentals=0),
    )


def early(window, place, lo, hi, side, own_w, peer_w, keep, windows, rows, half):
    ch = lo.shape[-1]
    width = half + 2 * EDGE
    chained = keep is not None
    return pl.pallas_call(
        functools.partial(early_kernel, window, chained),
        out_shape=(
            jax.ShapeDtypeStruct((windows, rows, 2 * half, ch), BF16),
            jax.ShapeDtypeStruct((rows, half, ch), BF16),
            jax.ShapeDtypeStruct((rows, width, ch), BF16),
        ),
        in_specs=[smem_spec()]
        + [vmem_spec()] * 3
        + [hbm_spec()] * 2
        + [any_spec()] * (1 if chained else 0),
        out_specs=(any_spec(), any_spec(), any_spec()),
        scratch_shapes=duo_scratch(rows, width, ch),
        input_output_aliases={6: 0} if chained else {},
        **duo_params(rows, width, ch),
    )(place, lo, hi, side, own_w, peer_w, *([keep] if chained else []))


def late(window, place, above, main, below, own_w, peer_w, buffers):
    rows, width, ch = main.shape
    return pl.pallas_call(
        functools.partial(late_kernel, window),
        out_shape=tuple(jax.ShapeDtypeStruct(b.shape, b.dtype) for b in buffers),
        in_specs=[smem_spec()] + [vmem_spec()] * 3 + [hbm_spec()] * 2 + [any_spec()] * 2,
        out_specs=(any_spec(), any_spec()),
        scratch_shapes=duo_scratch(rows, width, ch),
        input_output_aliases={6: 0, 7: 1},
        **duo_params(rows, width, ch),
    )(place, above, main, below, own_w, peer_w, *buffers)


def shards(features, weight_first, weight_second, weight_down, section_weights):
    segments = lax.axis_size("segment")
    strips = lax.axis_size("strip")
    seg = lax.axis_index("segment")
    strip = lax.axis_index("strip")
    windows, tile_rows, tile_cols, c1 = features.shape
    c2 = weight_down.shape[3]
    group = strips // segments
    strip_rows = segments * tile_rows // 2 // strips
    total_cols = strips * tile_cols // 2
    half = total_cols // 2
    core = lax.rem(seg, 2)
    far = seg // 2
    i32 = jnp.int32

    def device(s, c):
        return s * strips + c

    own_w = section_weights.reshape(3, 3 * c2, c2)
    peer_w = lax.ppermute(own_w, "segment", [(s, s ^ 1) for s in range(segments)])

    rim_r, rim_c = 6, 2
    ahead = [(s, s + 1) for s in range(segments - 1)]
    back = [(b, a) for a, b in ahead]
    top, bottom, first_cols, last_cols = pack(features, rim_r, rim_c)
    up = lax.ppermute(bottom, "segment", ahead)
    down = lax.ppermute(top, "segment", back)

    def side(cols, sl):
        ends = [jnp.swapaxes(rim[:, :, sl], 1, 2) for rim in (up, down)]
        return jnp.concatenate([cols, *ends], axis=2)

    along = [(c, c + 1) for c in range(strips - 1)]
    against = [(b, a) for a, b in along]
    left = lax.ppermute(
        side(last_cols, slice(tile_cols - rim_c, tile_cols)), "strip", along
    )
    right = lax.ppermute(side(first_cols, slice(0, rim_c)), "strip", against)

    stem_place = jnp.stack(
        [
            seg * tile_rows - rim_r,
            i32(segments * tile_rows),
            (strip == 0).astype(i32),
            (strip == strips - 1).astype(i32),
        ]
    ).astype(i32)
    w1, w2, wd = (
        pltpu.with_memory_space_constraint(w, pltpu.HBM)
        for w in (
            weight_first.reshape(3, 3 * c1, c1),
            weight_second.reshape(3, 3 * c1, c1),
            weight_down.reshape(4 * c1, c2),
        )
    )

    groups = [[g * group + i for i in range(group)] for g in range(segments)]
    low, high, edge = [], [], []
    for s in range(segments):
        for d in range(segments):
            for b in range(group):
                src, dst = device(s, d * group + b), device(d // 2, s * group + b)
                (low if d % 2 == 0 else high).append((src, dst))
                if d == 2:
                    edge.append((src, device(0, s * group + b)))
                if d == 1:
                    edge.append((src, device(1, s * group + b)))
    quarter = strip // group

    tiles = []
    for w in range(windows):
        z = stem(w, stem_place, features, up, down, left, right, w1, w2, wd, group)
        shape = z.shape
        got = lax.all_to_all(
            z.reshape(-1, *shape[2:]), "strip", 0, 0, axis_index_groups=groups, tiled=True
        ).reshape(shape)
        lo = lax.ppermute(got, AXES, low)
        hi = lax.ppermute(got, AXES, high)
        pick = lax.dynamic_index_in_dim(got, jnp.where(quarter == 2, 0, group - 1), 0, False)
        tiles.append((lo, hi, lax.ppermute(pick, AXES, edge)))

    common = [
        core,
        strip * strip_rows - 2,
        i32(segments * tile_rows // 2),
        core * half - EDGE,
        i32(total_cols),
    ]
    early_place = jnp.stack([(far == 0).astype(i32), *common]).astype(i32)
    late_place = jnp.stack([(far == 1).astype(i32), *common]).astype(i32)

    keep = None
    sends, passed = [], []
    across = [(device(h, t), device(h + 2, t)) for h in range(2) for t in range(strips)]
    for w in range(windows):
        keep, send, full = early(
            w, early_place, *tiles[w], own_w, peer_w, keep, windows, strip_rows, half
        )
        sends.append(send)
        passed.append(lax.ppermute(full, AXES, across))
    later = [(device(s, a), device(s, b)) for s in (2, 3) for a, b in along]
    sooner = [(b, a) for a, b in later]
    others = []
    for w in range(windows):
        main = passed[w]
        above = lax.ppermute(main[strip_rows - 2 :], AXES, later)
        below = lax.ppermute(main[:2], AXES, sooner)
        keep, send = late(
            w, late_place, above, main, below, own_w, peer_w, (keep, sends[w])
        )
        others.append(
            lax.ppermute(send, "segment", [(s, s ^ 1) for s in range(segments)])
        )
    zero = i32(0)
    for w in range(windows):
        keep = lax.dynamic_update_slice(
            keep, others[w][None], (i32(w), zero, (1 - core) * half, zero)
        )
    return keep[None]


def solution(mesh):
    return jax.shard_map(
        shards,
        mesh=mesh,
        in_specs=(
            P(None, "segment", "strip", None),
            P(),
            P(),
            P(),
            P("segment", None, None, None, None),
        ),
        out_specs=P("segment", None, "strip", None, None),
        check_vma=False,
    )
```

```python
import functools

import jax
import jax.numpy as jnp
from jax import lax
from jax.experimental import pallas as pl
from jax.experimental.pallas import tpu as pltpu
from jax.sharding import PartitionSpec as P

AXES = ("segment", "strip")
F32 = jnp.float32
BF16 = jnp.bfloat16
VMEM = pltpu.VMEM


def vmem_spec():
    return pl.BlockSpec(memory_space=pltpu.VMEM)


def smem_spec():
    return pl.BlockSpec(memory_space=pltpu.SMEM)


def hbm_spec():
    return pl.BlockSpec(memory_space=pltpu.HBM)


def any_spec():
    return pl.BlockSpec(memory_space=pl.ANY)


def pack_kernel(feat, top, bottom, first_cols, last_cols, wide):
    windows, rows, cols, ch = feat.shape
    rim_r, rim_c = top.shape[1], first_cols.shape[1]
    lanes = wide.shape[2]
    top[...] = feat[:, :rim_r]
    bottom[...] = feat[:, rows - rim_r :]
    for k in range(ch // lanes):
        at = slice(k * lanes, (k + 1) * lanes)
        wide[k] = feat[:, :, :, at].astype(F32).reshape(windows * rows * cols, lanes)
        for w in range(windows):
            for j in range(rim_c):
                base = w * rows * cols
                first_cols[w, j, :, at] = wide[k, pl.ds(base + j, rows, stride=cols), :].astype(BF16)
                last_cols[w, j, :, at] = wide[
                    k, pl.ds(base + cols - rim_c + j, rows, stride=cols), :
                ].astype(BF16)


def pack(features, rim_r, rim_c):
    windows, rows, cols, ch = features.shape
    row_shape = jax.ShapeDtypeStruct((windows, rim_r, cols, ch), BF16)
    col_shape = jax.ShapeDtypeStruct((windows, rim_c, rows, ch), BF16)
    return pl.pallas_call(
        pack_kernel,
        out_shape=(row_shape, row_shape, col_shape, col_shape),
        in_specs=[vmem_spec()],
        out_specs=(vmem_spec(),) * 4,
        scratch_shapes=[VMEM((ch // 128, windows * rows * cols, 128), F32)],
        compiler_params=pltpu.CompilerParams(vmem_limit_bytes=24 * 2**20),
        name="pack",
    )(features)


def stem_kernel(window, place, feat, up, down, left, right, w1_in, w2_in, wd_in, out, *scratch):
    s1, x1, s2, x2, s3, dbuf, w1, w2, wd, sems = scratch
    pairs = ((w1_in, w1), (w2_in, w2), (wd_in, wd))
    copies = [pltpu.make_async_copy(*pair, sems.at[i]) for i, pair in enumerate(pairs)]
    for copy in copies:
        copy.start()
    halo = 6
    _, rows, cols, ch = feat.shape
    full = rows + 2 * halo
    row_base = place[0]
    total_rows = place[1]
    left_edge = place[2]
    right_edge = place[3]
    pitch = s1.shape[1] // full
    width = cols + 8
    lanes = s1.shape[2]

    s1d = s1.reshape(ch // lanes, full, pitch, lanes)
    for k in range(ch // lanes):
        at = slice(k * lanes, (k + 1) * lanes)
        s1d[k, 0:halo, 8 : 8 + cols, :] = up[window, :, :, at].astype(F32)
        s1d[k, halo : halo + rows, 8 : 8 + cols, :] = feat[window, :, :, at].astype(F32)
        s1d[k, halo + rows : full, 8 : 8 + cols, :] = down[window, :, :, at].astype(F32)
        for src, to in ((left, 6), (right, 8 + cols)):
            for j in range(2):
                for take, put, count in (
                    (0, halo, rows),
                    (rows, 0, halo),
                    (rows + halo, halo + rows, halo),
                ):
                    s1[k, pl.ds(put * pitch + to + j, count, stride=pitch), :] = src[
                        window, j, take : take + count, at
                    ].astype(F32)

    step = 19

    def shift1(i, carry):
        r = i * step
        for c in range(3):
            for k in range(ch // lanes):
                x1[pl.ds(r, step), :, c * ch + k * lanes : c * ch + (k + 1) * lanes] = s1d[
                    k, pl.ds(r, step), 6 + c : 6 + c + width, :
                ].astype(BF16)
        return carry

    lax.fori_loop(0, full // step, shift1, 0)
    copies[0].wait()

    out1 = full - 2
    block1 = 37
    s2d = s2.reshape(out1, pitch, ch)

    def layer1(i, carry):
        r = i * block1
        acc = None
        for a in range(3):
            part = jnp.dot(
                x1[pl.ds(r + a, block1)].reshape(block1 * width, 3 * ch),
                w1[a],
                preferred_element_type=F32,
            )
            acc = part if acc is None else acc + part
        acc = acc.reshape(block1, width, ch)
        y = jnp.maximum(acc + x1[pl.ds(r + 1, block1), :, ch : 2 * ch].astype(F32), 0.0)
        row = row_base + 1 + r + lax.broadcasted_iota(jnp.int32, (block1, width, 1), 0)
        col = lax.broadcasted_iota(jnp.int32, (block1, width, 1), 1) - 1
        ok = (row >= 0) & (row < total_rows)
        ok = ok & ((col >= 0) | (left_edge == 0)) & ((col < cols) | (right_edge == 0))
        y = jnp.where(ok, y, 0.0)
        s2d[pl.ds(r, block1), 8 : 8 + width, :] = y.astype(BF16).astype(F32)
        return carry

    lax.fori_loop(0, out1 // block1, layer1, 0)

    def shift2(i, carry):
        r = i * block1
        for c in range(3):
            x2[pl.ds(r, block1), :, c * ch : (c + 1) * ch] = s2d[
                pl.ds(r, block1), 8 + c : 8 + c + cols, :
            ].astype(BF16)
        return carry

    lax.fori_loop(0, out1 // block1, shift2, 0)
    copies[1].wait()

    out2 = out1 - 2
    block2 = 36

    def layer2(i, carry):
        r = i * block2
        acc = None
        for a in range(3):
            part = jnp.dot(
                x2[pl.ds(r + a, block2)].reshape(block2 * cols, 3 * ch),
                w2[a],
                preferred_element_type=F32,
            )
            acc = part if acc is None else acc + part
        res = x2[pl.ds(r + 1, block2), :, ch : 2 * ch].reshape(block2 * cols, ch).astype(F32)
        y = jnp.maximum(acc + res, 0.0)
        y = y.astype(BF16).astype(F32)
        for k in range(ch // lanes):
            s3[k, pl.ds(i * (block2 * cols), block2 * cols), :] = y[:, k * lanes : (k + 1) * lanes]
        return carry

    lax.fori_loop(0, out2 // block2, layer2, 0)

    zrows = out2 // 2
    zcols = cols // 2

    for a in range(2):
        for c in range(2):
            for k in range(ch // lanes):
                at = (a * 2 + c) * ch + k * lanes
                for i in range(zrows):
                    dbuf[i * zcols : (i + 1) * zcols, at : at + lanes] = s3[
                        k, pl.ds((2 * i + a) * cols + c, zcols, stride=2), :
                    ].astype(BF16)
    copies[2].wait()
    z = jnp.maximum(jnp.dot(dbuf[...], wd[...], preferred_element_type=F32), 0.0)
    z = z.reshape(zrows, zcols, z.shape[-1])
    zrow = row_base // 2 + 1 + lax.broadcasted_iota(jnp.int32, (zrows, zcols, 1), 0)
    z = jnp.where((zrow >= 0) & (zrow < total_rows // 2), z, 0.0).astype(BF16)
    slots = out.shape[0]
    depth = out.shape[1]
    own = (zrows - 4) // slots
    for b in range(slots):
        out[b] = z[own * b : own * b + depth]


def stem(window, place, feat, up, down, left, right, w1, w2, wd, slots):
    _, rows, cols, ch = feat.shape
    full = rows + 12
    out_ch = wd.shape[1]
    own = rows // 2 // slots
    flops = 2 * (74 * 24 + 72 * 16) * 9 * ch * ch
    return pl.pallas_call(
        functools.partial(stem_kernel, window),
        out_shape=jax.ShapeDtypeStruct((slots, own + 4, cols // 2, out_ch), BF16),
        in_specs=[smem_spec()] + [vmem_spec()] * 5 + [hbm_spec()] * 3,
        out_specs=vmem_spec(),
        scratch_shapes=[
            VMEM((ch // 128, full * 32, 128), F32),
            VMEM((full, 24, 3 * ch), BF16),
            VMEM(((full - 2) * 32, ch), F32),
            VMEM((full - 2, 16, 3 * ch), BF16),
            VMEM((ch // 128, (full - 4) * 16, 128), F32),
            VMEM(((full - 4) // 2 * 8, 4 * ch), BF16),
            VMEM(w1.shape, BF16),
            VMEM(w2.shape, BF16),
            VMEM(wd.shape, BF16),
            pltpu.SemaphoreType.DMA((3,)),
        ],
        compiler_params=pltpu.CompilerParams(vmem_limit_bytes=48 * 2**20),
        cost_estimate=pl.CostEstimate(flops=flops, bytes_accessed=4 * 2**20, transcendentals=0),
    )(place, feat, up, down, left, right, w1, w2, wd)


EDGE = 8


def duo_body(place, fill, own_w, peer_w, keep, send, full, scratch, window):
    s1, x1, s2, x2, wa, wb, za, zb, zf, sems = scratch
    core = place[1]

    def load(mine, dst, taps, sem):
        @pl.when(core == mine)
        def _():
            pltpu.make_async_copy(own_w.at[taps], dst.at[taps], sem).start()

        @pl.when(core != mine)
        def _():
            pltpu.make_async_copy(peer_w.at[taps], dst.at[taps], sem).start()

    def tap_ready(a):
        pltpu.make_async_copy(own_w.at[pl.ds(a, 1)], wa.at[pl.ds(a, 1)], sems.at[3 + a]).wait()

    for a in range(3):
        load(0, wa, pl.ds(a, 1), sems.at[3 + a])
    inner = pl.multiple_of(core * EDGE, EDGE)
    row0, row_total, col0, col_total = place[2], place[3], place[4], place[5]
    rows_in, width, wide = x1.shape
    ch = wide // 3
    fill(s1)

    def shift(src, dst):
        def go(r, carry):
            for c in range(3):
                dst[r, :, c * ch : (c + 1) * ch] = src[
                    r, EDGE - 1 + c : EDGE - 1 + c + width, :
                ].astype(BF16)
            return carry

        lax.fori_loop(0, dst.shape[0], go, 0)

    def layer(x, w, r, first_row, ready=None):
        acc = None
        for a in range(3):
            if ready is not None:
                ready(a)
            part = jnp.dot(
                x[pl.ds(r + a, 2)].reshape(2 * width, 3 * ch), w[a], preferred_element_type=F32
            )
            acc = part if acc is None else acc + part
        acc = acc.reshape(2, width, ch)
        y = jnp.maximum(acc + x[pl.ds(r + 1, 2), :, ch : 2 * ch].astype(F32), 0.0)
        row = first_row + r + lax.broadcasted_iota(jnp.int32, (2, width, 1), 0)
        col = col0 + lax.broadcasted_iota(jnp.int32, (2, width, 1), 1)
        ok = (row >= 0) & (row < row_total) & (col >= 0) & (col < col_total)
        return jnp.where(ok, y, 0.0).astype(BF16)

    shift(s1, x1)
    rows_mid = rows_in - 2

    def first(i, carry, ready=None):
        r = 2 * i
        y = layer(x1, wa, r, row0 + 1, ready)
        s2[pl.ds(r, 2), EDGE : EDGE + width, :] = y.astype(F32)
        return carry

    first(0, 0, tap_ready)
    load(1, wb, pl.ds(0, 3), sems.at[6])
    lax.fori_loop(1, rows_mid // 2, first, 0)
    shift(s2, x2)
    rows_out = rows_mid - 2
    half = width - EDGE
    left_half, right_half = pl.ds(0, half), pl.ds(half, half)
    za[...] = x2[1 : 1 + rows_out, pl.ds(inner, half), ch : 2 * ch]

    @pl.when(core == 0)
    def _():
        pltpu.make_async_copy(za, keep.at[window, :, left_half, :], sems.at[0]).start()

    @pl.when(core == 1)
    def _():
        pltpu.make_async_copy(za, send, sems.at[0]).start()

    pltpu.make_async_copy(own_w, wb, sems.at[6]).wait()

    def second(i, carry):
        r = 2 * i
        two = pl.ds(r, 2)
        zf[two] = layer(x2, wb, r, row0 + 2)
        if full is not None:
            pltpu.make_async_copy(zf.at[two], full.at[two], sems.at[2]).start()
        zb[two] = zf[two, pl.ds(inner, half), :]

        @pl.when(core == 0)
        def _():
            pltpu.make_async_copy(zb.at[two], send.at[two], sems.at[1]).start()

        @pl.when(core == 1)
        def _():
            pltpu.make_async_copy(
                zb.at[two], keep.at[window, two, right_half, :], sems.at[1]
            ).start()

        return carry

    lax.fori_loop(0, rows_out // 2, second, 0)

    @pl.when(core == 0)
    def _():
        pltpu.make_async_copy(za, keep.at[window, :, left_half, :], sems.at[0]).wait()
        pltpu.make_async_copy(zb, send, sems.at[1]).wait()

    @pl.when(core == 1)
    def _():
        pltpu.make_async_copy(za, send, sems.at[0]).wait()
        pltpu.make_async_copy(zb, keep.at[window, :, right_half, :], sems.at[1]).wait()

    if full is not None:
        pltpu.make_async_copy(zf, full, sems.at[2]).wait()


def clear_edges(s, width):
    rows = s.shape[0]
    s[:, 0:EDGE, :] = jnp.zeros((rows, EDGE, s.shape[2]), F32)
    s[:, EDGE + width :, :] = jnp.zeros((rows, EDGE, s.shape[2]), F32)


def early_kernel(window, chained, *refs):
    place, lo, hi, side, own_w, peer_w = refs[:6]
    refs = refs[6 + (1 if chained else 0) :]
    keep, send, full = refs[:3]
    scratch = refs[3:]
    x1, s2 = scratch[1], scratch[2]
    width = x1.shape[1]
    block = lo.shape[2]

    def fill(s):
        clear_edges(s, width)
        clear_edges(s2, width)
        parts = lo.shape[0]

        core = place[1]
        base = EDGE + core * EDGE
        rim = pl.ds(pl.multiple_of(EDGE + (1 - core) * 2 * parts * block, EDGE), EDGE)

        def row(r, carry):
            for e in range(parts):
                at = pl.multiple_of(base + block * e, EDGE)
                s[r, pl.ds(at, block), :] = lo[e, r].astype(F32)
                at = pl.multiple_of(base + block * (e + parts), EDGE)
                s[r, pl.ds(at, block), :] = hi[e, r].astype(F32)
            s[r, rim, :] = side[r].astype(F32)
            return carry

        lax.fori_loop(0, s.shape[0], row, 0)

    @pl.when(place[0] == 1)
    def _():
        duo_body(place, fill, own_w, peer_w, keep, send, full, scratch, window)


def late_kernel(window, *refs):
    place, above, main, below, own_w, peer_w, _, _ = refs[:8]
    keep, send = refs[8:10]
    scratch = refs[10:]
    x1, s2 = scratch[1], scratch[2]
    width = x1.shape[1]

    def fill(s):
        clear_edges(s, width)
        clear_edges(s2, width)
        rim = above.shape[0]
        mid = main.shape[0]
        s[0:rim, EDGE : EDGE + width, :] = above[...].astype(F32)
        s[rim : rim + mid, EDGE : EDGE + width, :] = main[...].astype(F32)
        s[rim + mid :, EDGE : EDGE + width, :] = below[...].astype(F32)

    @pl.when(place[0] == 1)
    def _():
        duo_body(place, fill, own_w, peer_w, keep, send, None, scratch, window)


def duo_scratch(rows, width, ch):
    return [
        VMEM((rows + 4, width + 2 * EDGE, ch), F32),
        VMEM((rows + 4, width, 3 * ch), BF16),
        VMEM((rows + 2, width + 2 * EDGE, ch), F32),
        VMEM((rows + 2, width, 3 * ch), BF16),
        VMEM((3, 3 * ch, ch), BF16),
        VMEM((3, 3 * ch, ch), BF16),
        VMEM((rows, width - EDGE, ch), BF16),
        VMEM((rows, width - EDGE, ch), BF16),
        VMEM((rows, width, ch), BF16),
        pltpu.SemaphoreType.DMA((7,)),
    ]


def duo_params(rows, width, ch):
    flops = 2 * (2 * rows + 2) * width * 9 * ch * ch
    return dict(
        compiler_params=pltpu.CompilerParams(vmem_limit_bytes=48 * 2**20),
        cost_estimate=pl.CostEstimate(flops=flops, bytes_accessed=12 * 2**20, transcendentals=0),
    )


def early(window, place, lo, hi, side, own_w, peer_w, keep, windows, rows, half):
    ch = lo.shape[-1]
    width = half + EDGE
    chained = keep is not None
    return pl.pallas_call(
        functools.partial(early_kernel, window, chained),
        out_shape=(
            jax.ShapeDtypeStruct((windows, rows, 2 * half, ch), BF16),
            jax.ShapeDtypeStruct((rows, half, ch), BF16),
            jax.ShapeDtypeStruct((rows, width, ch), BF16),
        ),
        in_specs=[smem_spec()]
        + [vmem_spec()] * 3
        + [hbm_spec()] * 2
        + [any_spec()] * (1 if chained else 0),
        out_specs=(any_spec(), any_spec(), any_spec()),
        scratch_shapes=duo_scratch(rows, width, ch),
        input_output_aliases={6: 0} if chained else {},
        **duo_params(rows, width, ch),
    )(place, lo, hi, side, own_w, peer_w, *([keep] if chained else []))


def late(window, place, above, main, below, own_w, peer_w, buffers):
    rows, width, ch = main.shape
    return pl.pallas_call(
        functools.partial(late_kernel, window),
        out_shape=tuple(jax.ShapeDtypeStruct(b.shape, b.dtype) for b in buffers),
        in_specs=[smem_spec()] + [vmem_spec()] * 3 + [hbm_spec()] * 2 + [any_spec()] * 2,
        out_specs=(any_spec(), any_spec()),
        scratch_shapes=duo_scratch(rows, width, ch),
        input_output_aliases={6: 0, 7: 1},
        **duo_params(rows, width, ch),
    )(place, above, main, below, own_w, peer_w, *buffers)


def shards(features, weight_first, weight_second, weight_down, section_weights):
    segments = lax.axis_size("segment")
    strips = lax.axis_size("strip")
    seg = lax.axis_index("segment")
    strip = lax.axis_index("strip")
    windows, tile_rows, tile_cols, c1 = features.shape
    c2 = weight_down.shape[3]
    group = strips // segments
    strip_rows = segments * tile_rows // 2 // strips
    total_cols = strips * tile_cols // 2
    half = total_cols // 2
    core = lax.rem(seg, 2)
    far = seg // 2
    i32 = jnp.int32

    def device(s, c):
        return s * strips + c

    own_w = section_weights.reshape(3, 3 * c2, c2)
    peer_w = lax.ppermute(own_w, "segment", [(s, s ^ 1) for s in range(segments)])

    rim_r, rim_c = 6, 2
    ahead = [(s, s + 1) for s in range(segments - 1)]
    back = [(b, a) for a, b in ahead]
    top, bottom, first_cols, last_cols = pack(features, rim_r, rim_c)
    up = lax.ppermute(bottom, "segment", ahead)
    down = lax.ppermute(top, "segment", back)

    def side(cols, sl):
        ends = [jnp.swapaxes(rim[:, :, sl], 1, 2) for rim in (up, down)]
        return jnp.concatenate([cols, *ends], axis=2)

    along = [(c, c + 1) for c in range(strips - 1)]
    against = [(b, a) for a, b in along]
    left = lax.ppermute(
        side(last_cols, slice(tile_cols - rim_c, tile_cols)), "strip", along
    )
    right = lax.ppermute(side(first_cols, slice(0, rim_c)), "strip", against)

    stem_place = jnp.stack(
        [
            seg * tile_rows - rim_r,
            i32(segments * tile_rows),
            (strip == 0).astype(i32),
            (strip == strips - 1).astype(i32),
        ]
    ).astype(i32)
    w1, w2, wd = (
        pltpu.with_memory_space_constraint(w, pltpu.HBM)
        for w in (
            weight_first.reshape(3, 3 * c1, c1),
            weight_second.reshape(3, 3 * c1, c1),
            weight_down.reshape(4 * c1, c2),
        )
    )

    groups = [[g * group + i for i in range(group)] for g in range(segments)]
    low, high, edge = [], [], []
    for s in range(segments):
        for d in range(segments):
            for b in range(group):
                src, dst = device(s, d * group + b), device(d // 2, s * group + b)
                (low if d % 2 == 0 else high).append((src, dst))
                if d == 2:
                    edge.append((src, device(0, s * group + b)))
                if d == 1:
                    edge.append((src, device(1, s * group + b)))
    quarter = strip // group

    tiles = []
    for w in range(windows):
        z = stem(w, stem_place, features, up, down, left, right, w1, w2, wd, group)
        shape = z.shape
        got = lax.all_to_all(
            z.reshape(-1, *shape[2:]), "strip", 0, 0, axis_index_groups=groups, tiled=True
        ).reshape(shape)
        lo = lax.ppermute(got, AXES, low)
        hi = lax.ppermute(got, AXES, high)
        pick = lax.dynamic_index_in_dim(got, jnp.where(quarter == 2, 0, group - 1), 0, False)
        tiles.append((lo, hi, lax.ppermute(pick, AXES, edge)))

    common = [
        core,
        strip * strip_rows - 2,
        i32(segments * tile_rows // 2),
        core * (half - EDGE),
        i32(total_cols),
    ]
    early_place = jnp.stack([(far == 0).astype(i32), *common]).astype(i32)
    late_place = jnp.stack([(far == 1).astype(i32), *common]).astype(i32)

    keep = None
    sends, passed = [], []
    across = [(device(h, t), device(h + 2, t)) for h in range(2) for t in range(strips)]
    for w in range(windows):
        keep, send, full = early(
            w, early_place, *tiles[w], own_w, peer_w, keep, windows, strip_rows, half
        )
        sends.append(send)
        passed.append(lax.ppermute(full, AXES, across))
    later = [(device(s, a), device(s, b)) for s in (2, 3) for a, b in along]
    sooner = [(b, a) for a, b in later]
    others = []
    for w in range(windows):
        main = passed[w]
        above = lax.ppermute(main[strip_rows - 2 :], AXES, later)
        below = lax.ppermute(main[:2], AXES, sooner)
        keep, send = late(
            w, late_place, above, main, below, own_w, peer_w, (keep, sends[w])
        )
        others.append(
            lax.ppermute(send, "segment", [(s, s ^ 1) for s in range(segments)])
        )
    zero = i32(0)
    for w in range(windows):
        keep = lax.dynamic_update_slice(
            keep, others[w][None], (i32(w), zero, (1 - core) * half, zero)
        )
    return keep[None]


def solution(mesh):
    return jax.shard_map(
        shards,
        mesh=mesh,
        in_specs=(
            P(None, "segment", "strip", None),
            P(),
            P(),
            P(),
            P("segment", None, None, None, None),
        ),
        out_specs=P("segment", None, "strip", None, None),
        check_vma=False,
    )
```

```python
import functools

import jax
import jax.numpy as jnp
from jax import lax
from jax.experimental import pallas as pl
from jax.experimental.pallas import tpu as pltpu
from jax.sharding import PartitionSpec as P

AXES = ("segment", "strip")
F32 = jnp.float32
BF16 = jnp.bfloat16
VMEM = pltpu.VMEM


def vmem_spec():
    return pl.BlockSpec(memory_space=pltpu.VMEM)


def smem_spec():
    return pl.BlockSpec(memory_space=pltpu.SMEM)


def hbm_spec():
    return pl.BlockSpec(memory_space=pltpu.HBM)


def any_spec():
    return pl.BlockSpec(memory_space=pl.ANY)


def pack_kernel(feat, top, bottom, first_cols, last_cols, wide):
    windows, rows, cols, ch = feat.shape
    rim_r, rim_c = top.shape[1], first_cols.shape[1]
    lanes = wide.shape[2]
    top[...] = feat[:, :rim_r]
    bottom[...] = feat[:, rows - rim_r :]
    for k in range(ch // lanes):
        at = slice(k * lanes, (k + 1) * lanes)
        wide[k] = feat[:, :, :, at].astype(F32).reshape(windows * rows * cols, lanes)
        for w in range(windows):
            for j in range(rim_c):
                base = w * rows * cols
                first_cols[w, j, :, at] = wide[k, pl.ds(base + j, rows, stride=cols), :].astype(BF16)
                last_cols[w, j, :, at] = wide[
                    k, pl.ds(base + cols - rim_c + j, rows, stride=cols), :
                ].astype(BF16)


def pack(features, rim_r, rim_c):
    windows, rows, cols, ch = features.shape
    row_shape = jax.ShapeDtypeStruct((windows, rim_r, cols, ch), BF16)
    col_shape = jax.ShapeDtypeStruct((windows, rim_c, rows, ch), BF16)
    return pl.pallas_call(
        pack_kernel,
        out_shape=(row_shape, row_shape, col_shape, col_shape),
        in_specs=[vmem_spec()],
        out_specs=(vmem_spec(),) * 4,
        scratch_shapes=[VMEM((ch // 128, windows * rows * cols, 128), F32)],
        compiler_params=pltpu.CompilerParams(vmem_limit_bytes=24 * 2**20),
        name="pack",
    )(features)


def stem_kernel(window, place, feat, up, down, left, right, w1_in, w2_in, wd_in, out, *scratch):
    s1, x1, s2, x2, s3, dbuf, w1, w2, wd, sems = scratch
    pairs = ((w1_in, w1), (w2_in, w2), (wd_in, wd))
    copies = [pltpu.make_async_copy(*pair, sems.at[i]) for i, pair in enumerate(pairs)]
    for copy in copies:
        copy.start()
    halo = 6
    _, rows, cols, ch = feat.shape
    full = rows + 2 * halo
    row_base = place[0]
    total_rows = place[1]
    left_edge = place[2]
    right_edge = place[3]
    pitch = s1.shape[1] // full
    width = cols + 8
    lanes = s1.shape[2]

    s1d = s1.reshape(ch // lanes, full, pitch, lanes)
    for k in range(ch // lanes):
        at = slice(k * lanes, (k + 1) * lanes)
        s1d[k, 0:halo, 8 : 8 + cols, :] = up[window, :, :, at].astype(F32)
        s1d[k, halo : halo + rows, 8 : 8 + cols, :] = feat[window, :, :, at].astype(F32)
        s1d[k, halo + rows : full, 8 : 8 + cols, :] = down[window, :, :, at].astype(F32)
        for src, to in ((left, 6), (right, 8 + cols)):
            for j in range(2):
                for take, put, count in (
                    (0, halo, rows),
                    (rows, 0, halo),
                    (rows + halo, halo + rows, halo),
                ):
                    s1[k, pl.ds(put * pitch + to + j, count, stride=pitch), :] = src[
                        window, j, take : take + count, at
                    ].astype(F32)

    step = 19

    def shift1(i, carry):
        r = i * step
        for c in range(3):
            for k in range(ch // lanes):
                x1[pl.ds(r, step), :, c * ch + k * lanes : c * ch + (k + 1) * lanes] = s1d[
                    k, pl.ds(r, step), 6 + c : 6 + c + width, :
                ].astype(BF16)
        return carry

    lax.fori_loop(0, full // step, shift1, 0)
    copies[0].wait()

    out1 = full - 2
    block1 = 37
    s2d = s2.reshape(out1, pitch, ch)

    def layer1(i, carry):
        r = i * block1
        acc = None
        for a in range(3):
            part = jnp.dot(
                x1[pl.ds(r + a, block1)].reshape(block1 * width, 3 * ch),
                w1[a],
                preferred_element_type=F32,
            )
            acc = part if acc is None else acc + part
        acc = acc.reshape(block1, width, ch)
        y = jnp.maximum(acc + x1[pl.ds(r + 1, block1), :, ch : 2 * ch].astype(F32), 0.0)
        row = row_base + 1 + r + lax.broadcasted_iota(jnp.int32, (block1, width, 1), 0)
        col = lax.broadcasted_iota(jnp.int32, (block1, width, 1), 1) - 1
        ok = (row >= 0) & (row < total_rows)
        ok = ok & ((col >= 0) | (left_edge == 0)) & ((col < cols) | (right_edge == 0))
        y = jnp.where(ok, y, 0.0)
        s2d[pl.ds(r, block1), 8 : 8 + width, :] = y.astype(BF16).astype(F32)
        return carry

    lax.fori_loop(0, out1 // block1, layer1, 0)

    def shift2(i, carry):
        r = i * block1
        for c in range(3):
            x2[pl.ds(r, block1), :, c * ch : (c + 1) * ch] = s2d[
                pl.ds(r, block1), 8 + c : 8 + c + cols, :
            ].astype(BF16)
        return carry

    lax.fori_loop(0, out1 // block1, shift2, 0)
    copies[1].wait()

    out2 = out1 - 2
    block2 = 36

    def layer2(i, carry):
        r = i * block2
        acc = None
        for a in range(3):
            part = jnp.dot(
                x2[pl.ds(r + a, block2)].reshape(block2 * cols, 3 * ch),
                w2[a],
                preferred_element_type=F32,
            )
            acc = part if acc is None else acc + part
        res = x2[pl.ds(r + 1, block2), :, ch : 2 * ch].reshape(block2 * cols, ch).astype(F32)
        y = jnp.maximum(acc + res, 0.0)
        y = y.astype(BF16).astype(F32)
        for k in range(ch // lanes):
            s3[k, pl.ds(i * (block2 * cols), block2 * cols), :] = y[:, k * lanes : (k + 1) * lanes]
        return carry

    lax.fori_loop(0, out2 // block2, layer2, 0)

    zrows = out2 // 2
    zcols = cols // 2

    for a in range(2):
        for c in range(2):
            for k in range(ch // lanes):
                at = (a * 2 + c) * ch + k * lanes
                for i in range(zrows):
                    dbuf[i * zcols : (i + 1) * zcols, at : at + lanes] = s3[
                        k, pl.ds((2 * i + a) * cols + c, zcols, stride=2), :
                    ].astype(BF16)
    copies[2].wait()
    z = jnp.maximum(jnp.dot(dbuf[...], wd[...], preferred_element_type=F32), 0.0)
    z = z.reshape(zrows, zcols, z.shape[-1])
    zrow = row_base // 2 + 1 + lax.broadcasted_iota(jnp.int32, (zrows, zcols, 1), 0)
    z = jnp.where((zrow >= 0) & (zrow < total_rows // 2), z, 0.0).astype(BF16)
    slots = out.shape[0]
    depth = out.shape[1]
    own = (zrows - 4) // slots
    for b in range(slots):
        out[b] = z[own * b : own * b + depth]


def stem(window, place, feat, up, down, left, right, w1, w2, wd, slots):
    _, rows, cols, ch = feat.shape
    full = rows + 12
    out_ch = wd.shape[1]
    own = rows // 2 // slots
    flops = 2 * (74 * 24 + 72 * 16) * 9 * ch * ch
    return pl.pallas_call(
        functools.partial(stem_kernel, window),
        out_shape=jax.ShapeDtypeStruct((slots, own + 4, cols // 2, out_ch), BF16),
        in_specs=[smem_spec()] + [vmem_spec()] * 5 + [hbm_spec()] * 3,
        out_specs=vmem_spec(),
        scratch_shapes=[
            VMEM((ch // 128, full * 32, 128), F32),
            VMEM((full, 24, 3 * ch), BF16),
            VMEM(((full - 2) * 32, ch), F32),
            VMEM((full - 2, 16, 3 * ch), BF16),
            VMEM((ch // 128, (full - 4) * 16, 128), F32),
            VMEM(((full - 4) // 2 * 8, 4 * ch), BF16),
            VMEM(w1.shape, BF16),
            VMEM(w2.shape, BF16),
            VMEM(wd.shape, BF16),
            pltpu.SemaphoreType.DMA((3,)),
        ],
        compiler_params=pltpu.CompilerParams(vmem_limit_bytes=48 * 2**20),
        cost_estimate=pl.CostEstimate(flops=flops, bytes_accessed=4 * 2**20, transcendentals=0),
    )(place, feat, up, down, left, right, w1, w2, wd)


EDGE = 8


def duo_body(place, fill, own_w, peer_w, keep, send, full, scratch, window):
    s1, x1, s2, x2, wa, wb, za, zb, zf, sems = scratch
    core = place[1]

    def load(mine, dst, taps, sem):
        @pl.when(core == mine)
        def _():
            pltpu.make_async_copy(own_w.at[taps], dst.at[taps], sem).start()

        @pl.when(core != mine)
        def _():
            pltpu.make_async_copy(peer_w.at[taps], dst.at[taps], sem).start()

    def tap_ready(a):
        pltpu.make_async_copy(own_w.at[pl.ds(a, 1)], wa.at[pl.ds(a, 1)], sems.at[3 + a]).wait()

    for a in range(3):
        load(0, wa, pl.ds(a, 1), sems.at[3 + a])
    inner = pl.multiple_of(core * EDGE, EDGE)
    row0, row_total, col0, col_total = place[2], place[3], place[4], place[5]
    rows_in, width, wide = x1.shape
    ch = wide // 3
    fill(s1)

    def shift(src, dst):
        def go(r, carry):
            for c in range(3):
                dst[r, :, c * ch : (c + 1) * ch] = src[
                    r, EDGE - 1 + c : EDGE - 1 + c + width, :
                ].astype(BF16)
            return carry

        lax.fori_loop(0, dst.shape[0], go, 0)

    def layer(x, w, r, first_row, ready=None):
        acc = None
        for a in range(3):
            if ready is not None:
                ready(a)
            part = jnp.dot(
                x[pl.ds(r + a, 2)].reshape(2 * width, 3 * ch), w[a], preferred_element_type=F32
            )
            acc = part if acc is None else acc + part
        acc = acc.reshape(2, width, ch)
        y = jnp.maximum(acc + x[pl.ds(r + 1, 2), :, ch : 2 * ch].astype(F32), 0.0)
        row = first_row + r + lax.broadcasted_iota(jnp.int32, (2, width, 1), 0)
        col = col0 + lax.broadcasted_iota(jnp.int32, (2, width, 1), 1)
        ok = (row >= 0) & (row < row_total) & (col >= 0) & (col < col_total)
        return jnp.where(ok, y, 0.0).astype(BF16)

    shift(s1, x1)
    rows_mid = rows_in - 2

    def first(i, carry, ready=None):
        r = 2 * i
        y = layer(x1, wa, r, row0 + 1, ready)
        s2[pl.ds(r, 2), EDGE : EDGE + width, :] = y.astype(F32)
        return carry

    first(0, 0, tap_ready)
    load(1, wb, pl.ds(0, 3), sems.at[6])
    lax.fori_loop(1, rows_mid // 2, first, 0)
    shift(s2, x2)
    rows_out = rows_mid - 2
    half = width - EDGE
    left_half, right_half = pl.ds(0, half), pl.ds(half, half)
    za[...] = x2[1 : 1 + rows_out, pl.ds(inner, half), ch : 2 * ch]

    @pl.when(core == 0)
    def _():
        pltpu.make_async_copy(za, keep.at[window, :, left_half, :], sems.at[0]).start()

    @pl.when(core == 1)
    def _():
        pltpu.make_async_copy(za, send, sems.at[0]).start()

    pltpu.make_async_copy(own_w, wb, sems.at[6]).wait()

    def second(i, carry):
        r = 2 * i
        two = pl.ds(r, 2)
        zf[two] = layer(x2, wb, r, row0 + 2)
        for k, part in enumerate(full):

            @pl.when(i == k)
            def _(part=part):
                pltpu.make_async_copy(zf.at[two], part, sems.at[2]).start()

        zb[two] = zf[two, pl.ds(inner, half), :]

        @pl.when(core == 0)
        def _():
            pltpu.make_async_copy(zb.at[two], send.at[two], sems.at[1]).start()

        @pl.when(core == 1)
        def _():
            pltpu.make_async_copy(
                zb.at[two], keep.at[window, two, right_half, :], sems.at[1]
            ).start()

        return carry

    lax.fori_loop(0, rows_out // 2, second, 0)

    @pl.when(core == 0)
    def _():
        pltpu.make_async_copy(za, keep.at[window, :, left_half, :], sems.at[0]).wait()
        pltpu.make_async_copy(zb, send, sems.at[1]).wait()

    @pl.when(core == 1)
    def _():
        pltpu.make_async_copy(za, send, sems.at[0]).wait()
        pltpu.make_async_copy(zb, keep.at[window, :, right_half, :], sems.at[1]).wait()

    for k, part in enumerate(full):
        pltpu.make_async_copy(zf.at[pl.ds(2 * k, 2)], part, sems.at[2]).wait()


def clear_edges(s, width):
    rows = s.shape[0]
    s[:, 0:EDGE, :] = jnp.zeros((rows, EDGE, s.shape[2]), F32)
    s[:, EDGE + width :, :] = jnp.zeros((rows, EDGE, s.shape[2]), F32)


def early_kernel(window, chained, *refs):
    place, lo, hi, side, own_w, peer_w = refs[:6]
    refs = refs[6 + (1 if chained else 0) :]
    keep, send, *full = refs[:4]
    scratch = refs[4:]
    x1, s2 = scratch[1], scratch[2]
    width = x1.shape[1]
    block = lo.shape[2]

    def fill(s):
        clear_edges(s, width)
        clear_edges(s2, width)
        parts = lo.shape[0]

        core = place[1]
        base = EDGE + core * EDGE
        rim = pl.ds(pl.multiple_of(EDGE + (1 - core) * 2 * parts * block, EDGE), EDGE)

        def row(r, carry):
            for e in range(parts):
                at = pl.multiple_of(base + block * e, EDGE)
                s[r, pl.ds(at, block), :] = lo[e, r].astype(F32)
                at = pl.multiple_of(base + block * (e + parts), EDGE)
                s[r, pl.ds(at, block), :] = hi[e, r].astype(F32)
            s[r, rim, :] = side[r].astype(F32)
            return carry

        lax.fori_loop(0, s.shape[0], row, 0)

    @pl.when(place[0] == 1)
    def _():
        duo_body(place, fill, own_w, peer_w, keep, send, full, scratch, window)


def late_kernel(window, *refs):
    place, above, upper, lower, below, own_w, peer_w, _, _ = refs[:9]
    keep, send = refs[9:11]
    scratch = refs[11:]
    x1, s2 = scratch[1], scratch[2]
    width = x1.shape[1]

    def fill(s):
        clear_edges(s, width)
        clear_edges(s2, width)
        at = 0
        for piece in (above, upper, lower, below):
            s[at : at + piece.shape[0], EDGE : EDGE + width, :] = piece[...].astype(F32)
            at += piece.shape[0]

    @pl.when(place[0] == 1)
    def _():
        duo_body(place, fill, own_w, peer_w, keep, send, (), scratch, window)


def duo_scratch(rows, width, ch):
    return [
        VMEM((rows + 4, width + 2 * EDGE, ch), F32),
        VMEM((rows + 4, width, 3 * ch), BF16),
        VMEM((rows + 2, width + 2 * EDGE, ch), F32),
        VMEM((rows + 2, width, 3 * ch), BF16),
        VMEM((3, 3 * ch, ch), BF16),
        VMEM((3, 3 * ch, ch), BF16),
        VMEM((rows, width - EDGE, ch), BF16),
        VMEM((rows, width - EDGE, ch), BF16),
        VMEM((rows, width, ch), BF16),
        pltpu.SemaphoreType.DMA((7,)),
    ]


def duo_params(rows, width, ch):
    flops = 2 * (2 * rows + 2) * width * 9 * ch * ch
    return dict(
        compiler_params=pltpu.CompilerParams(vmem_limit_bytes=48 * 2**20),
        cost_estimate=pl.CostEstimate(flops=flops, bytes_accessed=12 * 2**20, transcendentals=0),
    )


def early(window, place, lo, hi, side, own_w, peer_w, keep, windows, rows, half):
    ch = lo.shape[-1]
    width = half + EDGE
    chained = keep is not None
    return pl.pallas_call(
        functools.partial(early_kernel, window, chained),
        out_shape=(
            jax.ShapeDtypeStruct((windows, rows, 2 * half, ch), BF16),
            jax.ShapeDtypeStruct((rows, half, ch), BF16),
            jax.ShapeDtypeStruct((rows // 2, width, ch), BF16),
            jax.ShapeDtypeStruct((rows // 2, width, ch), BF16),
        ),
        in_specs=[smem_spec()]
        + [vmem_spec()] * 3
        + [hbm_spec()] * 2
        + [any_spec()] * (1 if chained else 0),
        out_specs=(any_spec(),) * 4,
        scratch_shapes=duo_scratch(rows, width, ch),
        input_output_aliases={6: 0} if chained else {},
        **duo_params(rows, width, ch),
    )(place, lo, hi, side, own_w, peer_w, *([keep] if chained else []))


def late(window, place, above, upper, lower, below, own_w, peer_w, buffers):
    rows, width, ch = upper.shape
    rows *= 2
    return pl.pallas_call(
        functools.partial(late_kernel, window),
        out_shape=tuple(jax.ShapeDtypeStruct(b.shape, b.dtype) for b in buffers),
        in_specs=[smem_spec()] + [vmem_spec()] * 4 + [hbm_spec()] * 2 + [any_spec()] * 2,
        out_specs=(any_spec(), any_spec()),
        scratch_shapes=duo_scratch(rows, width, ch),
        input_output_aliases={7: 0, 8: 1},
        **duo_params(rows, width, ch),
    )(place, above, upper, lower, below, own_w, peer_w, *buffers)


def shards(features, weight_first, weight_second, weight_down, section_weights):
    segments = lax.axis_size("segment")
    strips = lax.axis_size("strip")
    seg = lax.axis_index("segment")
    strip = lax.axis_index("strip")
    windows, tile_rows, tile_cols, c1 = features.shape
    c2 = weight_down.shape[3]
    group = strips // segments
    strip_rows = segments * tile_rows // 2 // strips
    total_cols = strips * tile_cols // 2
    half = total_cols // 2
    core = lax.rem(seg, 2)
    far = seg // 2
    i32 = jnp.int32

    def device(s, c):
        return s * strips + c

    own_w = section_weights.reshape(3, 3 * c2, c2)
    peer_w = lax.ppermute(own_w, "segment", [(s, s ^ 1) for s in range(segments)])

    rim_r, rim_c = 6, 2
    ahead = [(s, s + 1) for s in range(segments - 1)]
    back = [(b, a) for a, b in ahead]
    top, bottom, first_cols, last_cols = pack(features, rim_r, rim_c)
    up = lax.ppermute(bottom, "segment", ahead)
    down = lax.ppermute(top, "segment", back)

    def side(cols, sl):
        ends = [jnp.swapaxes(rim[:, :, sl], 1, 2) for rim in (up, down)]
        return jnp.concatenate([cols, *ends], axis=2)

    along = [(c, c + 1) for c in range(strips - 1)]
    against = [(b, a) for a, b in along]
    left = lax.ppermute(
        side(last_cols, slice(tile_cols - rim_c, tile_cols)), "strip", along
    )
    right = lax.ppermute(side(first_cols, slice(0, rim_c)), "strip", against)

    stem_place = jnp.stack(
        [
            seg * tile_rows - rim_r,
            i32(segments * tile_rows),
            (strip == 0).astype(i32),
            (strip == strips - 1).astype(i32),
        ]
    ).astype(i32)
    w1, w2, wd = (
        pltpu.with_memory_space_constraint(w, pltpu.HBM)
        for w in (
            weight_first.reshape(3, 3 * c1, c1),
            weight_second.reshape(3, 3 * c1, c1),
            weight_down.reshape(4 * c1, c2),
        )
    )

    groups = [[g * group + i for i in range(group)] for g in range(segments)]
    low, high, edge = [], [], []
    for s in range(segments):
        for d in range(segments):
            for b in range(group):
                src, dst = device(s, d * group + b), device(d // 2, s * group + b)
                (low if d % 2 == 0 else high).append((src, dst))
                if d == 2:
                    edge.append((src, device(0, s * group + b)))
                if d == 1:
                    edge.append((src, device(1, s * group + b)))
    quarter = strip // group

    tiles = []
    for w in range(windows):
        z = stem(w, stem_place, features, up, down, left, right, w1, w2, wd, group)
        shape = z.shape
        got = lax.all_to_all(
            z.reshape(-1, *shape[2:]), "strip", 0, 0, axis_index_groups=groups, tiled=True
        ).reshape(shape)
        lo = lax.ppermute(got, AXES, low)
        hi = lax.ppermute(got, AXES, high)
        pick = lax.dynamic_index_in_dim(got, jnp.where(quarter == 2, 0, group - 1), 0, False)
        tiles.append((lo, hi, lax.ppermute(pick, AXES, edge)))

    common = [
        core,
        strip * strip_rows - 2,
        i32(segments * tile_rows // 2),
        core * (half - EDGE),
        i32(total_cols),
    ]
    early_place = jnp.stack([(far == 0).astype(i32), *common]).astype(i32)
    late_place = jnp.stack([(far == 1).astype(i32), *common]).astype(i32)

    keep = None
    sends, passed = [], []
    across = [(device(h, t), device(h + 2, t)) for h in range(2) for t in range(strips)]
    for w in range(windows):
        keep, send, *full = early(
            w, early_place, *tiles[w], own_w, peer_w, keep, windows, strip_rows, half
        )
        sends.append(send)
        passed.append([lax.ppermute(part, AXES, across) for part in full])
    later = [(device(s, a), device(s, b)) for s in (2, 3) for a, b in along]
    sooner = [(b, a) for a, b in later]
    others = []
    for w in range(windows):
        upper, lower = passed[w]
        above = lax.ppermute(lower, AXES, later)
        below = lax.ppermute(upper, AXES, sooner)
        keep, send = late(
            w, late_place, above, upper, lower, below, own_w, peer_w, (keep, sends[w])
        )
        others.append(
            lax.ppermute(send, "segment", [(s, s ^ 1) for s in range(segments)])
        )
    zero = i32(0)
    for w in range(windows):
        keep = lax.dynamic_update_slice(
            keep, others[w][None], (i32(w), zero, (1 - core) * half, zero)
        )
    return keep[None]


def solution(mesh):
    return jax.shard_map(
        shards,
        mesh=mesh,
        in_specs=(
            P(None, "segment", "strip", None),
            P(),
            P(),
            P(),
            P("segment", None, None, None, None),
        ),
        out_specs=P("segment", None, "strip", None, None),
        check_vma=False,
    )
```

```python
import functools

import jax
import jax.numpy as jnp
from jax import lax
from jax.experimental import pallas as pl
from jax.experimental.pallas import tpu as pltpu
from jax.sharding import PartitionSpec as P

AXES = ("segment", "strip")
F32 = jnp.float32
BF16 = jnp.bfloat16
VMEM = pltpu.VMEM


def vmem_spec():
    return pl.BlockSpec(memory_space=pltpu.VMEM)


def smem_spec():
    return pl.BlockSpec(memory_space=pltpu.SMEM)


def hbm_spec():
    return pl.BlockSpec(memory_space=pltpu.HBM)


def any_spec():
    return pl.BlockSpec(memory_space=pl.ANY)


def pack_kernel(feat, top, bottom, first_cols, last_cols, wide):
    windows, rows, cols, ch = feat.shape
    rim_r, rim_c = top.shape[1], first_cols.shape[1]
    lanes = wide.shape[2]
    top[...] = feat[:, :rim_r]
    bottom[...] = feat[:, rows - rim_r :]
    for k in range(ch // lanes):
        at = slice(k * lanes, (k + 1) * lanes)
        wide[k] = feat[:, :, :, at].astype(F32).reshape(windows * rows * cols, lanes)
        for w in range(windows):
            for j in range(rim_c):
                base = w * rows * cols
                first_cols[w, j, :, at] = wide[k, pl.ds(base + j, rows, stride=cols), :].astype(BF16)
                last_cols[w, j, :, at] = wide[
                    k, pl.ds(base + cols - rim_c + j, rows, stride=cols), :
                ].astype(BF16)


def pack(features, rim_r, rim_c):
    windows, rows, cols, ch = features.shape
    row_shape = jax.ShapeDtypeStruct((windows, rim_r, cols, ch), BF16)
    col_shape = jax.ShapeDtypeStruct((windows, rim_c, rows, ch), BF16)
    return pl.pallas_call(
        pack_kernel,
        out_shape=(row_shape, row_shape, col_shape, col_shape),
        in_specs=[vmem_spec()],
        out_specs=(vmem_spec(),) * 4,
        scratch_shapes=[VMEM((ch // 128, windows * rows * cols, 128), F32)],
        compiler_params=pltpu.CompilerParams(vmem_limit_bytes=24 * 2**20),
        name="pack",
    )(features)


def stem_kernel(window, place, feat, up, down, left, right, w1_in, w2_in, wd_in, out, *scratch):
    s1, x1, s2, x2, s3, dbuf, w1, w2, wd, sems = scratch
    pairs = ((w1_in, w1), (w2_in, w2), (wd_in, wd))
    copies = [pltpu.make_async_copy(*pair, sems.at[i]) for i, pair in enumerate(pairs)]
    for copy in copies:
        copy.start()
    halo = 6
    _, rows, cols, ch = feat.shape
    full = rows + 2 * halo
    row_base = place[0]
    total_rows = place[1]
    left_edge = place[2]
    right_edge = place[3]
    pitch = s1.shape[1] // full
    width = cols + 8
    lanes = s1.shape[2]

    s1d = s1.reshape(ch // lanes, full, pitch, lanes)
    for k in range(ch // lanes):
        at = slice(k * lanes, (k + 1) * lanes)
        s1d[k, 0:halo, 8 : 8 + cols, :] = up[window, :, :, at].astype(F32)
        s1d[k, halo : halo + rows, 8 : 8 + cols, :] = feat[window, :, :, at].astype(F32)
        s1d[k, halo + rows : full, 8 : 8 + cols, :] = down[window, :, :, at].astype(F32)
        for src, to in ((left, 6), (right, 8 + cols)):
            for j in range(2):
                for take, put, count in (
                    (0, halo, rows),
                    (rows, 0, halo),
                    (rows + halo, halo + rows, halo),
                ):
                    s1[k, pl.ds(put * pitch + to + j, count, stride=pitch), :] = src[
                        window, j, take : take + count, at
                    ].astype(F32)

    step = 19

    def shift1(i, carry):
        r = i * step
        for c in range(3):
            for k in range(ch // lanes):
                x1[pl.ds(r, step), :, c * ch + k * lanes : c * ch + (k + 1) * lanes] = s1d[
                    k, pl.ds(r, step), 6 + c : 6 + c + width, :
                ].astype(BF16)
        return carry

    lax.fori_loop(0, full // step, shift1, 0)
    copies[0].wait()

    out1 = full - 2
    block1 = 37
    s2d = s2.reshape(out1, pitch, ch)

    def layer1(i, carry):
        r = i * block1
        acc = None
        for a in range(3):
            part = jnp.dot(
                x1[pl.ds(r + a, block1)].reshape(block1 * width, 3 * ch),
                w1[a],
                preferred_element_type=F32,
            )
            acc = part if acc is None else acc + part
        acc = acc.reshape(block1, width, ch)
        y = jnp.maximum(acc + x1[pl.ds(r + 1, block1), :, ch : 2 * ch].astype(F32), 0.0)
        row = row_base + 1 + r + lax.broadcasted_iota(jnp.int32, (block1, width, 1), 0)
        col = lax.broadcasted_iota(jnp.int32, (block1, width, 1), 1) - 1
        ok = (row >= 0) & (row < total_rows)
        ok = ok & ((col >= 0) | (left_edge == 0)) & ((col < cols) | (right_edge == 0))
        y = jnp.where(ok, y, 0.0)
        s2d[pl.ds(r, block1), 8 : 8 + width, :] = y.astype(BF16).astype(F32)
        return carry

    lax.fori_loop(0, out1 // block1, layer1, 0)

    def shift2(i, carry):
        r = i * block1
        for c in range(3):
            x2[pl.ds(r, block1), :, c * ch : (c + 1) * ch] = s2d[
                pl.ds(r, block1), 8 + c : 8 + c + cols, :
            ].astype(BF16)
        return carry

    lax.fori_loop(0, out1 // block1, shift2, 0)
    copies[1].wait()

    out2 = out1 - 2
    block2 = 36

    def layer2(i, carry):
        r = i * block2
        acc = None
        for a in range(3):
            part = jnp.dot(
                x2[pl.ds(r + a, block2)].reshape(block2 * cols, 3 * ch),
                w2[a],
                preferred_element_type=F32,
            )
            acc = part if acc is None else acc + part
        res = x2[pl.ds(r + 1, block2), :, ch : 2 * ch].reshape(block2 * cols, ch).astype(F32)
        y = jnp.maximum(acc + res, 0.0)
        y = y.astype(BF16).astype(F32)
        for k in range(ch // lanes):
            s3[k, pl.ds(i * (block2 * cols), block2 * cols), :] = y[:, k * lanes : (k + 1) * lanes]
        return carry

    lax.fori_loop(0, out2 // block2, layer2, 0)

    zrows = out2 // 2
    zcols = cols // 2

    for a in range(2):
        for c in range(2):
            for k in range(ch // lanes):
                at = (a * 2 + c) * ch + k * lanes
                for i in range(zrows):
                    dbuf[i * zcols : (i + 1) * zcols, at : at + lanes] = s3[
                        k, pl.ds((2 * i + a) * cols + c, zcols, stride=2), :
                    ].astype(BF16)
    copies[2].wait()
    z = jnp.maximum(jnp.dot(dbuf[...], wd[...], preferred_element_type=F32), 0.0)
    z = z.reshape(zrows, zcols, z.shape[-1])
    zrow = row_base // 2 + 1 + lax.broadcasted_iota(jnp.int32, (zrows, zcols, 1), 0)
    z = jnp.where((zrow >= 0) & (zrow < total_rows // 2), z, 0.0).astype(BF16)
    slots = out.shape[0]
    depth = out.shape[1]
    own = (zrows - 4) // slots
    for b in range(slots):
        out[b] = z[own * b : own * b + depth]


def stem(window, place, feat, up, down, left, right, w1, w2, wd, slots):
    _, rows, cols, ch = feat.shape
    full = rows + 12
    out_ch = wd.shape[1]
    own = rows // 2 // slots
    flops = 2 * (74 * 24 + 72 * 16) * 9 * ch * ch
    return pl.pallas_call(
        functools.partial(stem_kernel, window),
        out_shape=jax.ShapeDtypeStruct((slots, own + 4, cols // 2, out_ch), BF16),
        in_specs=[smem_spec()] + [vmem_spec()] * 5 + [hbm_spec()] * 3,
        out_specs=vmem_spec(),
        scratch_shapes=[
            VMEM((ch // 128, full * 32, 128), F32),
            VMEM((full, 24, 3 * ch), BF16),
            VMEM(((full - 2) * 32, ch), F32),
            VMEM((full - 2, 16, 3 * ch), BF16),
            VMEM((ch // 128, (full - 4) * 16, 128), F32),
            VMEM(((full - 4) // 2 * 8, 4 * ch), BF16),
            VMEM(w1.shape, BF16),
            VMEM(w2.shape, BF16),
            VMEM(wd.shape, BF16),
            pltpu.SemaphoreType.DMA((3,)),
        ],
        compiler_params=pltpu.CompilerParams(vmem_limit_bytes=48 * 2**20),
        cost_estimate=pl.CostEstimate(flops=flops, bytes_accessed=4 * 2**20, transcendentals=0),
    )(place, feat, up, down, left, right, w1, w2, wd)


EDGE = 8


def duo_body(place, fill, own_w, peer_w, keep, send, full, scratch, window):
    s1, x1, s2, x2, wa, wb, za, zb, zf, sems = scratch
    core = place[1]

    def load(mine, dst, taps, sem):
        @pl.when(core == mine)
        def _():
            pltpu.make_async_copy(own_w.at[taps], dst.at[taps], sem).start()

        @pl.when(core != mine)
        def _():
            pltpu.make_async_copy(peer_w.at[taps], dst.at[taps], sem).start()

    def tap_ready(a):
        pltpu.make_async_copy(own_w.at[pl.ds(a, 1)], wa.at[pl.ds(a, 1)], sems.at[3 + a]).wait()

    for a in range(3):
        load(0, wa, pl.ds(a, 1), sems.at[3 + a])
    inner = pl.multiple_of(core * EDGE, EDGE)
    row0, row_total, col0, col_total = place[2], place[3], place[4], place[5]
    rows_in, width, wide = x1.shape
    ch = wide // 3
    fill(s1)

    def shift(src, dst):
        def go(r, carry):
            for c in range(3):
                dst[r, :, c * ch : (c + 1) * ch] = src[
                    r, EDGE - 1 + c : EDGE - 1 + c + width, :
                ].astype(BF16)
            return carry

        lax.fori_loop(0, dst.shape[0], go, 0)

    def layer(x, w, r, first_row, ready=None, cols=None):
        start, span = cols or (0, width)
        keep_cols = pl.ds(start, span)
        acc = None
        for a in range(3):
            if ready is not None:
                ready(a)
            part = jnp.dot(
                x[pl.ds(r + a, 2), keep_cols].reshape(2 * span, 3 * ch),
                w[a],
                preferred_element_type=F32,
            )
            acc = part if acc is None else acc + part
        acc = acc.reshape(2, span, ch)
        y = jnp.maximum(acc + x[pl.ds(r + 1, 2), keep_cols, ch : 2 * ch].astype(F32), 0.0)
        row = first_row + r + lax.broadcasted_iota(jnp.int32, (2, span, 1), 0)
        col = col0 + start + lax.broadcasted_iota(jnp.int32, (2, span, 1), 1)
        ok = (row >= 0) & (row < row_total) & (col >= 0) & (col < col_total)
        return jnp.where(ok, y, 0.0).astype(BF16)

    shift(s1, x1)
    rows_mid = rows_in - 2

    def first(i, carry, ready=None):
        r = 2 * i
        y = layer(x1, wa, r, row0 + 1, ready)
        s2[pl.ds(r, 2), EDGE : EDGE + width, :] = y.astype(F32)
        return carry

    first(0, 0, tap_ready)
    load(1, wb, pl.ds(0, 3), sems.at[6])
    lax.fori_loop(1, rows_mid // 2, first, 0)
    shift(s2, x2)
    rows_out = rows_mid - 2
    half = width - EDGE
    left_half, right_half = pl.ds(0, half), pl.ds(half, half)
    za[...] = x2[1 : 1 + rows_out, pl.ds(inner, half), ch : 2 * ch]

    @pl.when(core == 0)
    def _():
        pltpu.make_async_copy(za, keep.at[window, :, left_half, :], sems.at[0]).start()

    @pl.when(core == 1)
    def _():
        pltpu.make_async_copy(za, send, sems.at[0]).start()

    pltpu.make_async_copy(own_w, wb, sems.at[6]).wait()

    def second(i, carry):
        r = 2 * i
        two = pl.ds(r, 2)
        if full:
            zf[two] = layer(x2, wb, r, row0 + 2)
        for k, part in enumerate(full):

            @pl.when(i == k)
            def _(part=part):
                pltpu.make_async_copy(zf.at[two], part, sems.at[2]).start()

        if full:
            zb[two] = zf[two, pl.ds(inner, half), :]
        else:
            zb[two] = layer(x2, wb, r, row0 + 2, cols=(inner, half))

        @pl.when(core == 0)
        def _():
            pltpu.make_async_copy(zb.at[two], send.at[two], sems.at[1]).start()

        @pl.when(core == 1)
        def _():
            pltpu.make_async_copy(
                zb.at[two], keep.at[window, two, right_half, :], sems.at[1]
            ).start()

        return carry

    lax.fori_loop(0, rows_out // 2, second, 0)

    @pl.when(core == 0)
    def _():
        pltpu.make_async_copy(za, keep.at[window, :, left_half, :], sems.at[0]).wait()
        pltpu.make_async_copy(zb, send, sems.at[1]).wait()

    @pl.when(core == 1)
    def _():
        pltpu.make_async_copy(za, send, sems.at[0]).wait()
        pltpu.make_async_copy(zb, keep.at[window, :, right_half, :], sems.at[1]).wait()

    for k, part in enumerate(full):
        pltpu.make_async_copy(zf.at[pl.ds(2 * k, 2)], part, sems.at[2]).wait()


def clear_edges(s, width):
    rows = s.shape[0]
    s[:, 0:EDGE, :] = jnp.zeros((rows, EDGE, s.shape[2]), F32)
    s[:, EDGE + width :, :] = jnp.zeros((rows, EDGE, s.shape[2]), F32)


def early_kernel(window, chained, *refs):
    place, lo, hi, side, own_w, peer_w = refs[:6]
    refs = refs[6 + (1 if chained else 0) :]
    keep, send, *full = refs[:4]
    scratch = refs[4:]
    x1, s2 = scratch[1], scratch[2]
    width = x1.shape[1]
    block = lo.shape[2]

    def fill(s):
        clear_edges(s, width)
        clear_edges(s2, width)
        parts = lo.shape[0]

        core = place[1]
        base = EDGE + core * EDGE
        rim = pl.ds(pl.multiple_of(EDGE + (1 - core) * 2 * parts * block, EDGE), EDGE)

        def row(r, carry):
            for e in range(parts):
                at = pl.multiple_of(base + block * e, EDGE)
                s[r, pl.ds(at, block), :] = lo[e, r].astype(F32)
                at = pl.multiple_of(base + block * (e + parts), EDGE)
                s[r, pl.ds(at, block), :] = hi[e, r].astype(F32)
            s[r, rim, :] = side[r].astype(F32)
            return carry

        lax.fori_loop(0, s.shape[0], row, 0)

    @pl.when(place[0] == 1)
    def _():
        duo_body(place, fill, own_w, peer_w, keep, send, full, scratch, window)


def late_kernel(window, *refs):
    place, above, upper, lower, below, own_w, peer_w, _, _ = refs[:9]
    keep, send = refs[9:11]
    scratch = refs[11:]
    x1, s2 = scratch[1], scratch[2]
    width = x1.shape[1]

    def fill(s):
        clear_edges(s, width)
        clear_edges(s2, width)
        at = 0
        for piece in (above, upper, lower, below):
            s[at : at + piece.shape[0], EDGE : EDGE + width, :] = piece[...].astype(F32)
            at += piece.shape[0]

    @pl.when(place[0] == 1)
    def _():
        duo_body(place, fill, own_w, peer_w, keep, send, (), scratch, window)


def duo_scratch(rows, width, ch):
    return [
        VMEM((rows + 4, width + 2 * EDGE, ch), F32),
        VMEM((rows + 4, width, 3 * ch), BF16),
        VMEM((rows + 2, width + 2 * EDGE, ch), F32),
        VMEM((rows + 2, width, 3 * ch), BF16),
        VMEM((3, 3 * ch, ch), BF16),
        VMEM((3, 3 * ch, ch), BF16),
        VMEM((rows, width - EDGE, ch), BF16),
        VMEM((rows, width - EDGE, ch), BF16),
        VMEM((rows, width, ch), BF16),
        pltpu.SemaphoreType.DMA((7,)),
    ]


def duo_params(rows, width, ch):
    flops = 2 * (2 * rows + 2) * width * 9 * ch * ch
    return dict(
        compiler_params=pltpu.CompilerParams(vmem_limit_bytes=48 * 2**20),
        cost_estimate=pl.CostEstimate(flops=flops, bytes_accessed=12 * 2**20, transcendentals=0),
    )


def early(window, place, lo, hi, side, own_w, peer_w, keep, windows, rows, half):
    ch = lo.shape[-1]
    width = half + EDGE
    chained = keep is not None
    return pl.pallas_call(
        functools.partial(early_kernel, window, chained),
        out_shape=(
            jax.ShapeDtypeStruct((windows, rows, 2 * half, ch), BF16),
            jax.ShapeDtypeStruct((rows, half, ch), BF16),
            jax.ShapeDtypeStruct((rows // 2, width, ch), BF16),
            jax.ShapeDtypeStruct((rows // 2, width, ch), BF16),
        ),
        in_specs=[smem_spec()]
        + [vmem_spec()] * 3
        + [hbm_spec()] * 2
        + [any_spec()] * (1 if chained else 0),
        out_specs=(any_spec(),) * 4,
        scratch_shapes=duo_scratch(rows, width, ch),
        input_output_aliases={6: 0} if chained else {},
        **duo_params(rows, width, ch),
    )(place, lo, hi, side, own_w, peer_w, *([keep] if chained else []))


def late(window, place, above, upper, lower, below, own_w, peer_w, buffers):
    rows, width, ch = upper.shape
    rows *= 2
    return pl.pallas_call(
        functools.partial(late_kernel, window),
        out_shape=tuple(jax.ShapeDtypeStruct(b.shape, b.dtype) for b in buffers),
        in_specs=[smem_spec()] + [vmem_spec()] * 4 + [hbm_spec()] * 2 + [any_spec()] * 2,
        out_specs=(any_spec(), any_spec()),
        scratch_shapes=duo_scratch(rows, width, ch),
        input_output_aliases={7: 0, 8: 1},
        **duo_params(rows, width, ch),
    )(place, above, upper, lower, below, own_w, peer_w, *buffers)


def shards(features, weight_first, weight_second, weight_down, section_weights):
    segments = lax.axis_size("segment")
    strips = lax.axis_size("strip")
    seg = lax.axis_index("segment")
    strip = lax.axis_index("strip")
    windows, tile_rows, tile_cols, c1 = features.shape
    c2 = weight_down.shape[3]
    group = strips // segments
    strip_rows = segments * tile_rows // 2 // strips
    total_cols = strips * tile_cols // 2
    half = total_cols // 2
    core = lax.rem(seg, 2)
    far = seg // 2
    i32 = jnp.int32

    def device(s, c):
        return s * strips + c

    own_w = section_weights.reshape(3, 3 * c2, c2)
    peer_w = lax.ppermute(own_w, "segment", [(s, s ^ 1) for s in range(segments)])

    rim_r, rim_c = 6, 2
    ahead = [(s, s + 1) for s in range(segments - 1)]
    back = [(b, a) for a, b in ahead]
    top, bottom, first_cols, last_cols = pack(features, rim_r, rim_c)
    up = lax.ppermute(bottom, "segment", ahead)
    down = lax.ppermute(top, "segment", back)

    def side(cols, sl):
        ends = [jnp.swapaxes(rim[:, :, sl], 1, 2) for rim in (up, down)]
        return jnp.concatenate([cols, *ends], axis=2)

    along = [(c, c + 1) for c in range(strips - 1)]
    against = [(b, a) for a, b in along]
    left = lax.ppermute(
        side(last_cols, slice(tile_cols - rim_c, tile_cols)), "strip", along
    )
    right = lax.ppermute(side(first_cols, slice(0, rim_c)), "strip", against)

    stem_place = jnp.stack(
        [
            seg * tile_rows - rim_r,
            i32(segments * tile_rows),
            (strip == 0).astype(i32),
            (strip == strips - 1).astype(i32),
        ]
    ).astype(i32)
    w1, w2, wd = (
        pltpu.with_memory_space_constraint(w, pltpu.HBM)
        for w in (
            weight_first.reshape(3, 3 * c1, c1),
            weight_second.reshape(3, 3 * c1, c1),
            weight_down.reshape(4 * c1, c2),
        )
    )

    groups = [[g * group + i for i in range(group)] for g in range(segments)]
    low, high, edge = [], [], []
    for s in range(segments):
        for d in range(segments):
            for b in range(group):
                src, dst = device(s, d * group + b), device(d // 2, s * group + b)
                (low if d % 2 == 0 else high).append((src, dst))
                if d == 2:
                    edge.append((src, device(0, s * group + b)))
                if d == 1:
                    edge.append((src, device(1, s * group + b)))
    quarter = strip // group

    tiles = []
    for w in range(windows):
        z = stem(w, stem_place, features, up, down, left, right, w1, w2, wd, group)
        shape = z.shape
        got = lax.all_to_all(
            z.reshape(-1, *shape[2:]), "strip", 0, 0, axis_index_groups=groups, tiled=True
        ).reshape(shape)
        lo = lax.ppermute(got, AXES, low)
        hi = lax.ppermute(got, AXES, high)
        pick = lax.dynamic_index_in_dim(got, jnp.where(quarter == 2, 0, group - 1), 0, False)
        tiles.append((lo, hi, lax.ppermute(pick, AXES, edge)))

    common = [
        core,
        strip * strip_rows - 2,
        i32(segments * tile_rows // 2),
        core * (half - EDGE),
        i32(total_cols),
    ]
    early_place = jnp.stack([(far == 0).astype(i32), *common]).astype(i32)
    late_place = jnp.stack([(far == 1).astype(i32), *common]).astype(i32)

    keep = None
    sends, passed = [], []
    across = [(device(h, t), device(h + 2, t)) for h in range(2) for t in range(strips)]
    for w in range(windows):
        keep, send, *full = early(
            w, early_place, *tiles[w], own_w, peer_w, keep, windows, strip_rows, half
        )
        sends.append(send)
        passed.append([lax.ppermute(part, AXES, across) for part in full])
    later = [(device(s, a), device(s, b)) for s in (2, 3) for a, b in along]
    sooner = [(b, a) for a, b in later]
    others = []
    for w in range(windows):
        upper, lower = passed[w]
        above = lax.ppermute(lower, AXES, later)
        below = lax.ppermute(upper, AXES, sooner)
        keep, send = late(
            w, late_place, above, upper, lower, below, own_w, peer_w, (keep, sends[w])
        )
        others.append(
            lax.ppermute(send, "segment", [(s, s ^ 1) for s in range(segments)])
        )
    zero = i32(0)
    for w in range(windows):
        keep = lax.dynamic_update_slice(
            keep, others[w][None], (i32(w), zero, (1 - core) * half, zero)
        )
    return keep[None]


def solution(mesh):
    return jax.shard_map(
        shards,
        mesh=mesh,
        in_specs=(
            P(None, "segment", "strip", None),
            P(),
            P(),
            P(),
            P("segment", None, None, None, None),
        ),
        out_specs=P("segment", None, "strip", None, None),
        check_vma=False,
    )
```
